32 devices in a mesh: head: 16 (over z, y, core), dp: 2 (over x).
Axes of the slice: x: 2, y: 2, z: 4, core: 2. Of those that a mesh axis runs over, the one named last changes fastest.
Arguments:
- gradient_part: bfloat16 [2, 3, 4608, 2048], P('dp', None, None, 'head'), may hold values from -15 to 15
- carried_error: bfloat16 [2, 3, 4608, 2048], P('dp', None, None, 'head'), may hold values from -4 to 4
- query_basis: float32 [2048, 4], P('head'), may hold values from -6 to 6
Outputs:
- new_error: bfloat16 [2, 3, 4608, 2048], P('dp', None, None, 'head')
- compressed: float32 [2048, 4], P('head')
The draws below stay inside these ranges and needn't reach their ends.
All inputs are finite; a program needn't handle non-finite values.
Results may differ from the reference program's by a relative error of at most 0.008.
Values may be sent and summed in bfloat16 or wider, within the bound.
No kernel may reach another device: no remote copies, remote signals or barrier semaphores. Data moves between devices by JAX's collectives and lax.ppermute only.
A program may use at most 64 MiB of HBM per device.

```python
import jax
import jax.numpy as jnp
from jax import lax

D = 4608
RANK = 4
LAYERS = 3
COLUMNS = 2048
REPLICAS = 2


def draw_gradient_part(key, part):
    stacked_rows = LAYERS * D
    position = jnp.arange(stacked_rows, dtype=jnp.float32) / max(stacked_rows - 1, 1)
    low_scale = 0.4
    high_scale = 2.4
    values = jnp.clip(jax.random.normal(key, (REPLICAS, LAYERS, D, COLUMNS), jnp.float32), -6.0, 6.0)
    row_scale = jnp.exp(jnp.log(low_scale) + (jnp.log(high_scale) - jnp.log(low_scale)) * position)
    row_scale = row_scale.reshape(1, LAYERS, D, 1)
    return (values * row_scale).astype(jnp.bfloat16)


def levels(rng, shape, cuts, smallest, largest):
    level = 1.0
    for dim, blocks in cuts:
        heights = jax.random.uniform(jax.random.fold_in(jax.random.fold_in(rng, 6), dim), (blocks,), jnp.float32, smallest / len(cuts), largest / len(cuts))
        level = level * jnp.repeat(jnp.exp(heights), shape[dim] // blocks).reshape((-1,) + (1,) * (len(shape) - 1 - dim))
    return level


def centred(key, shape, width, most, cuts=(), kind=jnp.bfloat16):
    values = jax.random.normal(key, shape, jnp.float32) * width
    if len(cuts) > 0:
        values = levels(key, shape, cuts, -0.22, 0.18) * values
    return jnp.clip(values, min=-most, max=most).astype(kind)


def setup_inputs(seed: int = 0) -> dict:
    splits = jax.random.split(jax.random.key(seed), 4)
    gradient_part = draw_gradient_part(jax.random.fold_in(splits[3], 71), 0)
    carried_error = centred(splits[1], (REPLICAS, LAYERS, D, COLUMNS), 0.5, 4.0, ((0, 2), (3, 16)))
    query_basis = centred(splits[2], (COLUMNS, RANK), 1.0, 6.0, ((0, 16),), jnp.float32)
    return {"gradient_part": gradient_part, "carried_error": carried_error, "query_basis": query_basis}


def orthonormalize(projected):
    columns = []
    for column_index in range(RANK):
        initial = projected[:, column_index]
        vector = initial
        for earlier in columns:
            vector = vector - jnp.sum(earlier * initial) * earlier
        vector = vector / jnp.sqrt(jnp.sum(vector * vector))
        columns.append(vector)
    return jnp.stack(columns, axis=1)

def reference(gradient_part, carried_error, query_basis):
    stacked_rows = LAYERS * D

    def merged_of(replica):
        total = gradient_part[replica].astype(jnp.float32) + carried_error[replica].astype(jnp.float32)
        return total.reshape(stacked_rows, COLUMNS)
    projected = jnp.zeros((stacked_rows, RANK), jnp.float32)
    for replica in range(REPLICAS):
        projected = projected + jnp.dot(merged_of(replica), query_basis, precision=lax.Precision.HIGHEST)
    basis = orthonormalize(projected)
    compressed = jnp.zeros((COLUMNS, RANK), jnp.float32)
    for replica in range(REPLICAS):
        compressed = compressed + jnp.dot(merged_of(replica).T, basis, precision=lax.Precision.HIGHEST)
    compressed = compressed / REPLICAS
    approximation = jnp.dot(basis, compressed.T, precision=lax.Precision.HIGHEST)
    errors = []
    for replica in range(REPLICAS):
        remainder = (merged_of(replica) - approximation).astype(jnp.bfloat16)
        errors.append(remainder.reshape(LAYERS, D, COLUMNS))
    return (jnp.stack(errors, axis=0), compressed)
```

```python
import functools

import jax
import jax.numpy as jnp
from jax import lax
from jax.experimental import pallas as pl
from jax.experimental.pallas import tpu as pltpu
from jax.sharding import PartitionSpec as P

STREAMS = 2
FOLD = 2
LANES = 128
MIB = 1 << 20
BF16, F32 = jnp.bfloat16, jnp.float32


def split_bf16(x):
    high = x.astype(BF16)
    return high, (x - high.astype(F32)).astype(BF16)


def chunk_columns(run):
    tiles = run // LANES
    return LANES * max(t for t in range(1, 10) if tiles % t == 0)


def project_kernel(rank, g_hbm, e_hbm, q_ref, g_ref, e_ref, *rest):
    outs, sems = rest[:STREAMS], rest[STREAMS]
    rows = g_ref.shape[0]
    run = rows // (STREAMS * FOLD)
    cols = chunk_columns(run)
    order = [(s, k, t) for s in range(STREAMS) for k in range(run // cols) for t in range(FOLD)]
    copies = []
    for n, (s, k, t) in enumerate(order):
        at = pl.ds((s * FOLD + t) * run + k * cols, cols)
        pair = (
            pltpu.make_async_copy(g_hbm.at[at], g_ref.at[at], sems.at[0, n]),
            pltpu.make_async_copy(e_hbm.at[at], e_ref.at[at], sems.at[1, n]),
        )
        for copy in pair:
            copy.start()
        copies.append(pair)
    query = q_ref[...]
    high, low = split_bf16(query)
    high, low = high.astype(F32), low.astype(F32)
    zero = jnp.zeros((rank, LANES), F32)
    left = []
    for t in range(FOLD):
        parts = [zero] * (2 * FOLD)
        parts[t], parts[FOLD + t] = high, low
        part = jnp.concatenate(parts, axis=0).astype(BF16)
        left.append(jnp.concatenate([part, part], axis=1))
    for n, (s, k, t) in enumerate(order):
        for copy in copies[n]:
            copy.wait()
        at = pl.ds((s * FOLD + t) * run + k * cols, cols)
        both = jnp.concatenate([g_ref[at, :], e_ref[at, :]], axis=1)
        product = lax.dot_general(left[t], both, (((1,), (1,)), ((), ())), preferred_element_type=F32)
        half = FOLD * rank
        total = product[:half] + product[half:]
        to = pl.ds(k * cols, cols)
        if t == 0:
            held = total
        else:
            outs[s][:, to] = held + total


def project(gradient, error, query_t):
    rows, width = gradient.shape
    rank = query_t.shape[0]
    run = rows // (STREAMS * FOLD)
    steps = STREAMS * FOLD * (run // chunk_columns(run))
    stream = pltpu.VMEM((FOLD * rank, run), F32)
    return pl.pallas_call(
        functools.partial(project_kernel, rank),
        out_shape=(pltpu.VMEM((rows, width), BF16), pltpu.VMEM((rows, width), BF16)) + (stream,) * STREAMS,
        in_specs=[
            pl.BlockSpec(memory_space=pltpu.HBM),
            pl.BlockSpec(memory_space=pltpu.HBM),
            pl.BlockSpec(memory_space=pltpu.VMEM),
        ],
        out_specs=tuple(pl.BlockSpec(memory_space=pltpu.VMEM) for _ in range(2 + STREAMS)),
        scratch_shapes=[pltpu.SemaphoreType.DMA((2, steps))],
        compiler_params=pltpu.CompilerParams(vmem_limit_bytes=8 * MIB),
        name="project",
    )(
        pltpu.with_memory_space_constraint(gradient, pltpu.HBM),
        pltpu.with_memory_space_constraint(error, pltpu.HBM),
        query_t,
    )


def factor_kernel(rank, g_ref, e_ref, *rest):
    summed, received, (out_ref, gram_ref), streams = (
        rest[:STREAMS],
        rest[STREAMS : 2 * STREAMS],
        rest[2 * STREAMS : 2 * STREAMS + 2],
        rest[2 * STREAMS + 2 :],
    )
    carries = lax.rem(lax.axis_index("head"), 2) == 1
    rows = g_ref.shape[0]
    run = rows // (STREAMS * FOLD)
    cols = chunk_columns(run)
    half = FOLD * rank
    sums = [jnp.zeros((2 * half, 2 * LANES), F32) for _ in range(FOLD)]
    grams = [jnp.zeros((half, LANES), F32) for _ in range(rank)]
    for s in range(STREAMS):
        for k in range(run // cols):
            here = pl.ds(k * cols, cols)
            part = jnp.where(carries, summed[s][:, here], received[s][:, here])
            streams[s][:, here] = part
            high, low = split_bf16(part)
            left = jnp.concatenate([high.astype(F32), low.astype(F32)], axis=0).astype(BF16)
            for t in range(FOLD):
                at = pl.ds((s * FOLD + t) * run + k * cols, cols)
                both = jnp.concatenate([g_ref[at, :], e_ref[at, :]], axis=1)
                sums[t] += jnp.dot(left, both, preferred_element_type=F32)
            for d in range(rank):
                other = part if d == 0 else pltpu.roll(part, d, 0)
                product = part * other
                for c in range(cols // LANES):
                    grams[d] += product[:, c * LANES : (c + 1) * LANES]
    total = jnp.zeros((rank, LANES), F32)
    for t in range(FOLD):
        whole = sums[t][:, :LANES] + sums[t][:, LANES:]
        whole = whole[:half] + whole[half:]
        total += whole[t * rank : (t + 1) * rank]
    out_ref[...] = total
    for d in range(rank):
        gram_ref[d * half : (d + 1) * half, :] = jnp.broadcast_to(
            jnp.sum(grams[d], axis=1, keepdims=True), (half, LANES)
        )


def factor(gradient, error, summed, received, rank):
    width = gradient.shape[1]
    stream = pltpu.VMEM(summed[0].shape, F32)
    vmem = pl.BlockSpec(memory_space=pltpu.VMEM)
    return pl.pallas_call(
        functools.partial(factor_kernel, rank),
        out_shape=(pltpu.VMEM((rank, width), F32), pltpu.VMEM((rank * FOLD * rank, LANES), F32)) + (stream,) * STREAMS,
        in_specs=[vmem] * (2 + 2 * STREAMS),
        out_specs=(vmem,) * (2 + STREAMS),
        compiler_params=pltpu.CompilerParams(vmem_limit_bytes=8 * MIB),
        name="factor",
    )(gradient, error, *summed, *received)


def finish_kernel(rank, replicas, g_ref, e_ref, own_ref, peer_ref, gram_ref, *rest):
    streams = rest[:STREAMS]
    new_hbm, factor_ref, staged, sems = rest[STREAMS:]
    rows = g_ref.shape[0]
    run = rows // (STREAMS * FOLD)
    cols = chunk_columns(run)
    half = FOLD * rank

    def gram(i, j):
        d = i - j
        value = gram_ref[d * half + i : d * half + i + 1, :]
        for t in range(1, FOLD):
            row = d * half + t * rank + i
            value = value + gram_ref[row : row + 1, :]
        return value

    lower, inverse = {}, {}
    for j in range(rank):
        for i in range(j, rank):
            value = gram(i, j)
            for k in range(j):
                value = value - lower[i, k] * lower[j, k]
            if i == j:
                lower[j, j] = jnp.sqrt(value)
                inverse[j] = 1.0 / lower[j, j]
            else:
                lower[i, j] = value * inverse[j]
    raw = (own_ref[...] + peer_ref[...]) * (1.0 / replicas)
    small = []
    for j in range(rank):
        value = raw[j : j + 1]
        for k in range(j):
            value = value - lower[j, k] * small[k]
        small.append(value * inverse[j])
    factor_ref[...] = jnp.concatenate(small, axis=0)
    back = [None] * rank
    for j in reversed(range(rank)):
        value = small[j]
        for k in range(j + 1, rank):
            value = value - lower[k, j] * back[k]
        back[j] = value * inverse[j]
    weight = jnp.concatenate(back, axis=0)
    high, low = split_bf16(weight)
    high, low = high.astype(F32), low.astype(F32)
    zero = jnp.zeros((rank, LANES), F32)
    blocks = []
    for t in range(FOLD):
        def at_fold(x):
            return [x if u == t else zero for u in range(FOLD)]

        blocks.append(jnp.concatenate(at_fold(high) + at_fold(high) + at_fold(low) + [zero] * FOLD, axis=0))
    right = jnp.concatenate(blocks, axis=1).astype(BF16)
    copies = []
    for s in range(STREAMS):
        for k in range(run // cols):
            part = streams[s][:, pl.ds(k * cols, cols)]
            part_high, part_low = split_bf16(part)
            part_high, part_low = part_high.astype(F32), part_low.astype(F32)
            left = jnp.concatenate([part_high, part_low, part_high, jnp.zeros_like(part)], axis=0).astype(BF16)
            product = lax.dot_general(left, right, (((0,), (0,)), ((), ())), preferred_element_type=F32)
            for t in range(FOLD):
                at = pl.ds((s * FOLD + t) * run + k * cols, cols)
                merged = g_ref[at, :].astype(F32) + e_ref[at, :].astype(F32)
                staged[at, :] = (merged - product[:, t * LANES : (t + 1) * LANES]).astype(BF16)
                copy = pltpu.make_async_copy(staged.at[at], new_hbm.at[at], sems.at[len(copies)])
                copy.start()
                copies.append(copy)
    for copy in copies:
        copy.wait()


def finish(gradient, error, own, peer, gram, streams, rank, replicas):
    rows, width = gradient.shape
    run = rows // (STREAMS * FOLD)
    steps = STREAMS * FOLD * (run // chunk_columns(run))
    vmem = pl.BlockSpec(memory_space=pltpu.VMEM)
    return pl.pallas_call(
        functools.partial(finish_kernel, rank, replicas),
        out_shape=(jax.ShapeDtypeStruct((rows, width), BF16), jax.ShapeDtypeStruct((rank, width), F32)),
        in_specs=[vmem] * (5 + STREAMS),
        out_specs=(pl.BlockSpec(memory_space=pltpu.HBM), vmem),
        scratch_shapes=[pltpu.VMEM((rows, width), BF16), pltpu.SemaphoreType.DMA((steps,))],
        compiler_params=pltpu.CompilerParams(vmem_limit_bytes=12 * MIB),
        name="finish",
    )(gradient, error, own, peer, gram, *streams)


def exchange_plan(heads, replicas):
    carriers = [h * replicas + r for h in range(1, heads, 2) for r in range(replicas)]
    inward = [(i - replicas, i) for i in carriers]
    outward = [(i, i - replicas) for i in carriers]
    bits = []
    for bit in range(replicas.bit_length() - 1):
        bits.append(1 << bit)
    for bit in range(1, heads.bit_length() - 1):
        bits.append(replicas << bit)
    return inward, [[(i, i ^ bit) for i in carriers] for bit in bits], outward


def per_device(gradient_part, carried_error, query_basis):
    width = gradient_part.shape[3]
    rows = gradient_part.shape[1] * gradient_part.shape[2]
    rank = query_basis.shape[1]
    axes = ("head", "dp")
    heads, replicas = lax.axis_size("head"), lax.axis_size("dp")
    inward, stages, outward = exchange_plan(heads, replicas)
    gradient, error, *streams = project(
        gradient_part.reshape(rows, width), carried_error.reshape(rows, width), query_basis.T
    )
    summed, received = [], []
    for value in streams:
        value = value + lax.ppermute(value, axes, inward)
        for pairs in stages:
            value = value + lax.ppermute(value, axes, pairs)
        summed.append(value)
        received.append(lax.ppermute(value, axes, outward))
    own, gram, *done = factor(gradient, error, summed, received, rank)
    peer = jnp.zeros_like(own)
    total = own
    bit = 1
    while bit < replicas:
        peer = lax.ppermute(total, "dp", [(i, i ^ bit) for i in range(replicas)])
        own, total = total, total + peer
        bit *= 2
    new_error, compressed = finish(gradient, error, own, peer, gram, done, rank, replicas)
    return new_error.reshape(gradient_part.shape), compressed.T


def solution(mesh):
    in_specs = (P("dp", None, None, "head"), P("dp", None, None, "head"), P("head", None))
    out_specs = (P("dp", None, None, "head"), P("head", None))
    return jax.shard_map(
        per_device, mesh=mesh, in_specs=in_specs, out_specs=out_specs, check_vma=False
    )
```

```python
import functools

import jax
import jax.numpy as jnp
from jax import lax
from jax.experimental import pallas as pl
from jax.experimental.pallas import tpu as pltpu
from jax.sharding import PartitionSpec as P

STREAMS = 2
FOLD = 2
LANES = 128
MIB = 1 << 20
BF16, F32 = jnp.bfloat16, jnp.float32
VMEM = pl.BlockSpec(memory_space=pltpu.VMEM)
HBM = pl.BlockSpec(memory_space=pltpu.HBM)


def split_bf16(x):
    high = x.astype(BF16).astype(F32)
    return high, (x - high).astype(BF16).astype(F32)


def pieces(total, most):
    count = -(-total // most)
    ends = [total * i // count for i in range(count + 1)]
    return [(a * LANES, (b - a) * LANES) for a, b in zip(ends, ends[1:])]


def stream_pieces(run):
    tiles = run // LANES
    ends = [-(-tiles * i // STREAMS) for i in range(STREAMS + 1)]
    return [(a * LANES, (b - a) * LANES) for a, b in zip(ends, ends[1:])]


def kept_half():
    parity = 0
    for axis in ("head", "dp"):
        place = lax.axis_index(axis)
        for bit in range(lax.axis_size(axis).bit_length() - 1):
            parity = parity + lax.rem(place // (1 << bit), 2)
    return lax.rem(parity, 2)


def row_slice(half, fold, run, start, size):
    return pl.ds(pl.multiple_of(half * (FOLD * run) + (fold * run + start), LANES), size)


def project_kernel(rank, g_hbm, e_hbm, q_hbm, g_ref, e_ref, *rest):
    outs, (q_ref, sems, q_sem) = rest[: 2 * STREAMS], rest[2 * STREAMS :]
    run = g_ref.shape[0] // (2 * FOLD)
    kept = kept_half()
    query_copy = pltpu.make_async_copy(q_hbm, q_ref, q_sem)
    query_copy.start()
    order = []
    for part, half in enumerate((1 - kept, kept)):
        for s, (base, width) in enumerate(stream_pieces(run)):
            for start, size in pieces(width // LANES, 7):
                for fold in range(FOLD):
                    order.append((part * STREAMS + s, start, fold, row_slice(half, fold, run, base + start, size)))
    copies = []
    for n, (_, _, _, at) in enumerate(order):
        pair = (
            pltpu.make_async_copy(g_hbm.at[at], g_ref.at[at], sems.at[0, n]),
            pltpu.make_async_copy(e_hbm.at[at], e_ref.at[at], sems.at[1, n]),
        )
        for copy in pair:
            copy.start()
        copies.append(pair)
    query_copy.wait()
    high, low = split_bf16(q_ref[...])
    zero = jnp.zeros((rank, LANES), F32)
    left = []
    for fold in range(FOLD):
        parts = [zero] * (2 * FOLD)
        parts[fold], parts[FOLD + fold] = high, low
        part = jnp.concatenate(parts, axis=0).astype(BF16)
        left.append(jnp.concatenate([part, part], axis=1))
    held = None
    for n, (to, start, fold, at) in enumerate(order):
        for copy in copies[n]:
            copy.wait()
        both = jnp.concatenate([g_ref[at, :], e_ref[at, :]], axis=1)
        product = lax.dot_general(left[fold], both, (((1,), (1,)), ((), ())), preferred_element_type=F32)
        total = product[: FOLD * rank] + product[FOLD * rank :]
        held = total if fold == 0 else held + total
        if fold == FOLD - 1:
            outs[to][:, start : start + both.shape[0]] = held


def project(gradient, error, query_t):
    rows, width = gradient.shape
    rank = query_t.shape[0]
    run = rows // (2 * FOLD)
    streams = stream_pieces(run)
    steps = 2 * FOLD * sum(len(pieces(w // LANES, 7)) for _, w in streams)
    parts = tuple(pltpu.VMEM((FOLD * rank, w), F32) for _, w in streams)
    return pl.pallas_call(
        functools.partial(project_kernel, rank),
        out_shape=(pltpu.VMEM((rows, width), BF16),) * 2 + parts * 2,
        in_specs=[HBM] * 3,
        out_specs=(VMEM,) * (2 + 2 * STREAMS),
        scratch_shapes=[
            pltpu.VMEM((rank, width), F32),
            pltpu.SemaphoreType.DMA((2, steps)),
            pltpu.SemaphoreType.DMA,
        ],
        compiler_params=pltpu.CompilerParams(vmem_limit_bytes=4 * MIB),
        name="project",
    )(*(pltpu.with_memory_space_constraint(x, pltpu.HBM) for x in (gradient, error, query_t)))


def merge_kernel(g_ref, e_ref, out_ref):
    def step(i, _):
        at = pl.ds(pl.multiple_of(i * LANES, LANES), LANES)
        out_ref[at, :] = g_ref[at, :].astype(F32) + e_ref[at, :].astype(F32)
        return 0

    lax.fori_loop(0, g_ref.shape[0] // LANES, step, 0, unroll=2)


def merge(gradient, error):
    return pl.pallas_call(
        merge_kernel,
        out_shape=pltpu.VMEM(gradient.shape, F32),
        in_specs=[VMEM] * 2,
        out_specs=VMEM,
        compiler_params=pltpu.CompilerParams(vmem_limit_bytes=4 * MIB),
        name="merge",
    )(gradient, error)


def factor_kernel(rank, other, g_ref, e_ref, *rest):
    streams, so_far, (out_ref,) = rest[:STREAMS], rest[STREAMS:-1], rest[-1:]
    run = g_ref.shape[0] // (2 * FOLD)
    kept = kept_half()
    half = 1 - kept if other else kept
    sums = [jnp.zeros((2 * FOLD * rank, 2 * LANES), F32) for _ in range(FOLD)]
    for s, (base, width) in enumerate(stream_pieces(run)):
        for start, size in pieces(width // LANES, 7):
            left = jnp.concatenate(split_bf16(streams[s][:, start : start + size]), axis=0).astype(BF16)
            for fold in range(FOLD):
                at = row_slice(half, fold, run, base + start, size)
                both = jnp.concatenate([g_ref[at, :], e_ref[at, :]], axis=1)
                sums[fold] += jnp.dot(left, both, preferred_element_type=F32)
    total = so_far[0][...] if so_far else jnp.zeros((rank, LANES), F32)
    for fold in range(FOLD):
        whole = sums[fold][:, :LANES] + sums[fold][:, LANES:]
        whole = whole[: FOLD * rank] + whole[FOLD * rank :]
        total += whole[fold * rank : (fold + 1) * rank]
    out_ref[...] = total


def factor(gradient, error, streams, so_far, rank):
    width = gradient.shape[1]
    other = len(so_far) > 0
    return pl.pallas_call(
        functools.partial(factor_kernel, rank, other),
        out_shape=pltpu.VMEM((rank, width), F32),
        in_specs=[VMEM] * (2 + STREAMS + len(so_far)),
        out_specs=VMEM,
        compiler_params=pltpu.CompilerParams(vmem_limit_bytes=4 * MIB),
        name="factor_other" if other else "factor_kept",
    )(gradient, error, *streams, *so_far)


def solve(rank, replicas, gram, out_ref):
    lower, reciprocal = {}, {}
    for j in range(rank):
        for i in range(j, rank):
            value = gram(i, j)
            for k in range(j):
                value = value - lower[i, k] * lower[j, k]
            if i == j:
                reciprocal[j] = 1.0 / jnp.sqrt(value)
            else:
                lower[i, j] = value * reciprocal[j]
    inverse = {}
    for j in range(rank):
        inverse[j, j] = reciprocal[j]
        for i in range(j + 1, rank):
            value = lower[i, j] * inverse[j, j]
            for k in range(j + 1, i):
                value = value + lower[i, k] * inverse[k, j]
            inverse[i, j] = -value * reciprocal[i]
    zero = jnp.zeros((1, LANES), F32)
    for k in range(rank):
        for j in range(rank):
            column = inverse[j, k] * (1.0 / replicas) if j >= k else zero
            row = inverse[k, j] if k >= j else zero
            out_ref[8 * k + j : 8 * k + j + 1, :] = column
            out_ref[8 * (rank + k) + j : 8 * (rank + k) + j + 1, :] = row


def prepare_kernel(rank, replicas, other, *rest):
    streams, so_far, (left_ref, out_ref) = rest[:STREAMS], rest[STREAMS:-2], rest[-2:]
    rows = FOLD * rank
    run = left_ref.shape[0]
    grams = [jnp.zeros((rows, LANES), F32) for _ in range(rank)]
    for s, (base, width) in enumerate(stream_pieces(run)):
        for start, size in pieces(width // LANES, 7):
            part = streams[s][:, start : start + size]
            high, low = split_bf16(part)
            left = jnp.concatenate([high, low, high, jnp.zeros_like(part)], axis=0)
            left_ref[base + start : base + start + size, :] = left.T.astype(BF16)
            for d in range(rank):
                product = part * (part if d == 0 else pltpu.roll(part, d, 0))
                for c in range(0, size, LANES):
                    grams[d] += product[:, c : c + LANES]
    sums = []
    for d in range(rank):
        value = jnp.broadcast_to(jnp.sum(grams[d], axis=1, keepdims=True), (rows, LANES))
        sums.append(value + so_far[0][d * rows : (d + 1) * rows, :] if so_far else value)
    if not other:
        for d in range(rank):
            out_ref[d * rows : (d + 1) * rows, :] = sums[d]
        return

    def gram(i, j):
        return sum(sums[i - j][fold * rank + i : fold * rank + i + 1] for fold in range(FOLD))

    solve(rank, replicas, gram, out_ref)


def prepare(streams, so_far, run, rank, replicas):
    other = len(so_far) > 0
    out_rows = 16 * rank if other else rank * FOLD * rank
    return pl.pallas_call(
        functools.partial(prepare_kernel, rank, replicas, other),
        out_shape=(pltpu.VMEM((run, 4 * FOLD * rank), BF16), pltpu.VMEM((out_rows, LANES), F32)),
        in_specs=[VMEM] * (STREAMS + len(so_far)),
        out_specs=(VMEM,) * 2,
        compiler_params=pltpu.CompilerParams(vmem_limit_bytes=8 * MIB),
        name="prepare_other" if other else "prepare_kept",
    )(*streams, *so_far)


def finish_kernel(rank, merged_ref, kept_ref, other_ref, inverse_ref, own_ref, peer_ref, new_hbm, factor_ref, staged, sems):
    run = kept_ref.shape[0]
    kept = kept_half()
    raw = own_ref[...] + peer_ref[...]
    small = sum(inverse_ref[8 * k : 8 * k + rank, :] * raw[k : k + 1] for k in range(rank))
    factor_ref[...] = small
    weight = sum(inverse_ref[8 * (rank + k) : 8 * (rank + k) + rank, :] * small[k : k + 1] for k in range(rank))
    high, low = split_bf16(weight)
    zero = jnp.zeros((rank, LANES), F32)
    blocks = []
    for fold in range(FOLD):
        parts = [part if u == fold else zero for part in (high, high, low, zero) for u in range(FOLD)]
        blocks.append(jnp.concatenate(parts, axis=0))
    right = jnp.concatenate(blocks, axis=1).astype(BF16)
    copies = []
    for left_ref, half in ((kept_ref, kept), (other_ref, 1 - kept)):
        for start, size in pieces(run // LANES, 4):
            product = jnp.dot(left_ref[start : start + size, :], right, preferred_element_type=F32)
            for fold in range(FOLD):
                at = row_slice(half, fold, run, start, size)
                staged[at, :] = (merged_ref[at, :] - product[:, fold * LANES : (fold + 1) * LANES]).astype(BF16)
                copy = pltpu.make_async_copy(staged.at[at], new_hbm.at[at], sems.at[len(copies)])
                copy.start()
                copies.append(copy)
    for copy in copies:
        copy.wait()


def finish(merged, left_kept, left_other, inverse, own, peer):
    rows, width = merged.shape
    rank = own.shape[0]
    steps = 2 * FOLD * len(pieces(left_kept.shape[0] // LANES, 4))
    return pl.pallas_call(
        functools.partial(finish_kernel, rank),
        out_shape=(jax.ShapeDtypeStruct((rows, width), BF16), jax.ShapeDtypeStruct((rank, width), F32)),
        in_specs=[VMEM] * 6,
        out_specs=(HBM, VMEM),
        scratch_shapes=[pltpu.VMEM((rows, width), BF16), pltpu.SemaphoreType.DMA((steps,))],
        compiler_params=pltpu.CompilerParams(vmem_limit_bytes=8 * MIB),
        name="finish",
    )(merged, left_kept, left_other, inverse, own, peer)


def per_device(gradient_part, carried_error, query_basis):
    width = gradient_part.shape[3]
    rows = gradient_part.shape[1] * gradient_part.shape[2]
    rank = query_basis.shape[1]
    heads, replicas = lax.axis_size("head"), lax.axis_size("dp")

    def swap(x, bits):
        return lax.ppermute(x, ("head", "dp"), [(i, i ^ bits) for i in range(heads * replicas)])

    gradient, error, *parts = project(
        gradient_part.reshape(rows, width), carried_error.reshape(rows, width), query_basis.T
    )
    partner = replicas
    others = [1 << b for b in range((heads * replicas).bit_length() - 1) if 1 << b != partner]
    kept, other = [], []
    for s in range(STREAMS):
        turn = len(others) * s // STREAMS
        value = parts[STREAMS + s] + swap(parts[s], partner)
        for bit in others[turn:] + others[:turn]:
            value = value + swap(value, bit | partner)
        kept.append(value)
        other.append(swap(value, partner))
    merged = merge(gradient, error)
    own = factor(gradient, error, kept, (), rank)
    left_kept, gram = prepare(kept, (), rows // (2 * FOLD), rank, replicas)
    own = factor(gradient, error, other, (own,), rank)
    left_other, inverse = prepare(other, (gram,), rows // (2 * FOLD), rank, replicas)
    peer = jnp.zeros_like(own)
    total = own
    bit = 1
    while bit < replicas:
        peer = lax.ppermute(total, "dp", [(i, i ^ bit) for i in range(replicas)])
        own, total = total, total + peer
        bit *= 2
    new_error, compressed = finish(merged, left_kept, left_other, inverse, own, peer)
    return new_error.reshape(gradient_part.shape), compressed.T


def solution(mesh):
    in_specs = (P("dp", None, None, "head"), P("dp", None, None, "head"), P("head", None))
    out_specs = (P("dp", None, None, "head"), P("head", None))
    return jax.shard_map(
        per_device, mesh=mesh, in_specs=in_specs, out_specs=out_specs, check_vma=False
    )
```

```python
import functools

import jax
import jax.numpy as jnp
from jax import lax
from jax.experimental import pallas as pl
from jax.experimental.pallas import tpu as pltpu
from jax.sharding import PartitionSpec as P

STREAMS = 2
FOLD = 2
LANES = 128
MIB = 1 << 20
BF16, F32 = jnp.bfloat16, jnp.float32
VMEM = pl.BlockSpec(memory_space=pltpu.VMEM)
HBM = pl.BlockSpec(memory_space=pltpu.HBM)


def split_bf16(x):
    high = x.astype(BF16).astype(F32)
    return high, (x - high).astype(BF16).astype(F32)


def pieces(total, most):
    count = -(-total // most)
    ends = [total * i // count for i in range(count + 1)]
    return [(a * LANES, (b - a) * LANES) for a, b in zip(ends, ends[1:])]


def stream_pieces(run):
    tiles = run // LANES
    ends = [-(-tiles * i // STREAMS) for i in range(STREAMS + 1)]
    return [(a * LANES, (b - a) * LANES) for a, b in zip(ends, ends[1:])]


def kept_half():
    parity = 0
    for axis in ("head", "dp"):
        place = lax.axis_index(axis)
        for bit in range(lax.axis_size(axis).bit_length() - 1):
            parity = parity + lax.rem(place // (1 << bit), 2)
    return lax.rem(parity, 2)


def row_slice(half, fold, run, start, size):
    return pl.ds(pl.multiple_of(half * (FOLD * run) + (fold * run + start), LANES), size)


def project_half(half, left_ref, g_ref, e_ref, outs, ready):
    run = g_ref.shape[0] // (2 * FOLD)
    rows = left_ref.shape[0] // FOLD
    for fold in range(FOLD):
        ready(fold)
        at = row_slice(half, fold, run, 0, run)
        both = jnp.concatenate([g_ref[at, :], e_ref[at, :]], axis=1)
        left = left_ref[fold * rows : (fold + 1) * rows, :]
        product = lax.dot_general(left, both, (((1,), (1,)), ((), ())), preferred_element_type=F32)
        total = product[: rows // 2] + product[rows // 2 :]
        for out, (start, size) in zip(outs, stream_pieces(run)):
            part = total[:, start : start + size]
            out[...] = part if fold == 0 else out[...] + part


def project_sent_kernel(rank, g_hbm, e_hbm, q_hbm, g_ref, e_ref, left_ref, *rest):
    outs, (q_ref, sems, q_sem) = rest[:STREAMS], rest[STREAMS:]
    run = g_ref.shape[0] // (2 * FOLD)
    kept = kept_half()
    query_copy = pltpu.make_async_copy(q_hbm, q_ref, q_sem)
    query_copy.start()
    copies = []
    for part, half in enumerate((1 - kept, kept)):
        for fold in range(FOLD):
            at, n = row_slice(half, fold, run, 0, run), len(copies)
            pair = (
                pltpu.make_async_copy(g_hbm.at[at], g_ref.at[at], sems.at[0, n]),
                pltpu.make_async_copy(e_hbm.at[at], e_ref.at[at], sems.at[1, n]),
            )
            for copy in pair:
                copy.start()
            copies.append(pair)
    query_copy.wait()
    high, low = split_bf16(q_ref[...])
    zero = jnp.zeros((rank, LANES), F32)
    for fold in range(FOLD):
        parts = [part if u == fold else zero for part in (high, low) for u in range(FOLD)]
        part = jnp.concatenate(parts, axis=0).astype(BF16)
        rows = part.shape[0]
        left_ref[fold * rows : (fold + 1) * rows, :] = jnp.concatenate([part, part], axis=1)

    def ready(n):
        for copy in copies[n]:
            copy.wait()

    project_half(1 - kept, left_ref, g_ref, e_ref, outs, ready)
    for fold in range(FOLD):
        ready(FOLD + fold)


def project_sent(gradient, error, query_t):
    rows, width = gradient.shape
    rank = query_t.shape[0]
    parts = tuple(pltpu.VMEM((FOLD * rank, w), F32) for _, w in stream_pieces(rows // (2 * FOLD)))
    return pl.pallas_call(
        functools.partial(project_sent_kernel, rank),
        out_shape=(pltpu.VMEM((rows, width), BF16),) * 2 + (pltpu.VMEM((FOLD * 2 * FOLD * rank, 2 * width), BF16),) + parts,
        in_specs=[HBM] * 3,
        out_specs=(VMEM,) * (3 + STREAMS),
        scratch_shapes=[
            pltpu.VMEM((rank, width), F32),
            pltpu.SemaphoreType.DMA((2, 2 * FOLD)),
            pltpu.SemaphoreType.DMA,
        ],
        compiler_params=pltpu.CompilerParams(vmem_limit_bytes=4 * MIB),
        name="project_sent",
    )(*(pltpu.with_memory_space_constraint(x, pltpu.HBM) for x in (gradient, error, query_t)))


def project_kept_kernel(g_ref, e_ref, left_ref, *outs):
    project_half(kept_half(), left_ref, g_ref, e_ref, outs, lambda fold: None)


def project_kept(gradient, error, left):
    rows = left.shape[0] // FOLD
    parts = tuple(pltpu.VMEM((rows // 2, w), F32) for _, w in stream_pieces(gradient.shape[0] // (2 * FOLD)))
    return pl.pallas_call(
        project_kept_kernel,
        out_shape=parts,
        in_specs=[VMEM] * 3,
        out_specs=(VMEM,) * STREAMS,
        compiler_params=pltpu.CompilerParams(vmem_limit_bytes=4 * MIB),
        name="project_kept",
    )(gradient, error, left)


def merge_kernel(g_ref, e_ref, out_ref):
    def step(i, _):
        at = pl.ds(pl.multiple_of(i * LANES, LANES), LANES)
        out_ref[at, :] = g_ref[at, :].astype(F32) + e_ref[at, :].astype(F32)
        return 0

    lax.fori_loop(0, g_ref.shape[0] // LANES, step, 0, unroll=2)


def merge(gradient, error):
    return pl.pallas_call(
        merge_kernel,
        out_shape=pltpu.VMEM(gradient.shape, F32),
        in_specs=[VMEM] * 2,
        out_specs=VMEM,
        compiler_params=pltpu.CompilerParams(vmem_limit_bytes=4 * MIB),
        name="merge",
    )(gradient, error)


def factor_kernel(rank, other, g_ref, e_ref, *rest):
    streams, so_far, (out_ref,) = rest[:STREAMS], rest[STREAMS:-1], rest[-1:]
    run = g_ref.shape[0] // (2 * FOLD)
    kept = kept_half()
    half = 1 - kept if other else kept
    sums = [jnp.zeros((2 * FOLD * rank, 2 * LANES), F32) for _ in range(FOLD)]
    for s, (base, width) in enumerate(stream_pieces(run)):
        for start, size in pieces(width // LANES, 7):
            left = jnp.concatenate(split_bf16(streams[s][:, start : start + size]), axis=0).astype(BF16)
            for fold in range(FOLD):
                at = row_slice(half, fold, run, base + start, size)
                both = jnp.concatenate([g_ref[at, :], e_ref[at, :]], axis=1)
                sums[fold] += jnp.dot(left, both, preferred_element_type=F32)
    total = so_far[0][...] if so_far else jnp.zeros((rank, LANES), F32)
    for fold in range(FOLD):
        whole = sums[fold][:, :LANES] + sums[fold][:, LANES:]
        whole = whole[: FOLD * rank] + whole[FOLD * rank :]
        total += whole[fold * rank : (fold + 1) * rank]
    out_ref[...] = total


def factor(gradient, error, streams, so_far, rank):
    width = gradient.shape[1]
    other = len(so_far) > 0
    return pl.pallas_call(
        functools.partial(factor_kernel, rank, other),
        out_shape=pltpu.VMEM((rank, width), F32),
        in_specs=[VMEM] * (2 + STREAMS + len(so_far)),
        out_specs=VMEM,
        compiler_params=pltpu.CompilerParams(vmem_limit_bytes=4 * MIB),
        name="factor_other" if other else "factor_kept",
    )(gradient, error, *streams, *so_far)


def solve(rank, replicas, gram, out_ref):
    lower, reciprocal = {}, {}
    for j in range(rank):
        for i in range(j, rank):
            value = gram(i, j)
            for k in range(j):
                value = value - lower[i, k] * lower[j, k]
            if i == j:
                reciprocal[j] = 1.0 / jnp.sqrt(value)
            else:
                lower[i, j] = value * reciprocal[j]
    inverse = {}
    for j in range(rank):
        inverse[j, j] = reciprocal[j]
        for i in range(j + 1, rank):
            value = lower[i, j] * inverse[j, j]
            for k in range(j + 1, i):
                value = value + lower[i, k] * inverse[k, j]
            inverse[i, j] = -value * reciprocal[i]
    zero = jnp.zeros((1, LANES), F32)
    for k in range(rank):
        for j in range(rank):
            column = inverse[j, k] * (1.0 / replicas) if j >= k else zero
            row = inverse[k, j] if k >= j else zero
            out_ref[8 * k + j : 8 * k + j + 1, :] = column
            out_ref[8 * (rank + k) + j : 8 * (rank + k) + j + 1, :] = row


def prepare_kernel(rank, replicas, other, *rest):
    streams, so_far, (left_ref, out_ref) = rest[:STREAMS], rest[STREAMS:-2], rest[-2:]
    rows = FOLD * rank
    run = left_ref.shape[0]
    grams = [jnp.zeros((rows, LANES), F32) for _ in range(rank)]
    for s, (base, width) in enumerate(stream_pieces(run)):
        for start, size in pieces(width // LANES, 7):
            part = streams[s][:, start : start + size]
            high, low = split_bf16(part)
            left = jnp.concatenate([high, low, high, jnp.zeros_like(part)], axis=0)
            left_ref[base + start : base + start + size, :] = left.T.astype(BF16)
            for d in range(rank):
                product = part * (part if d == 0 else pltpu.roll(part, d, 0))
                for c in range(0, size, LANES):
                    grams[d] += product[:, c : c + LANES]
    sums = []
    for d in range(rank):
        value = jnp.broadcast_to(jnp.sum(grams[d], axis=1, keepdims=True), (rows, LANES))
        sums.append(value + so_far[0][d * rows : (d + 1) * rows, :] if so_far else value)
    if not other:
        for d in range(rank):
            out_ref[d * rows : (d + 1) * rows, :] = sums[d]
        return

    def gram(i, j):
        return sum(sums[i - j][fold * rank + i : fold * rank + i + 1] for fold in range(FOLD))

    solve(rank, replicas, gram, out_ref)


def prepare(streams, so_far, run, rank, replicas):
    other = len(so_far) > 0
    out_rows = 16 * rank if other else rank * FOLD * rank
    return pl.pallas_call(
        functools.partial(prepare_kernel, rank, replicas, other),
        out_shape=(pltpu.VMEM((run, 4 * FOLD * rank), BF16), pltpu.VMEM((out_rows, LANES), F32)),
        in_specs=[VMEM] * (STREAMS + len(so_far)),
        out_specs=(VMEM,) * 2,
        compiler_params=pltpu.CompilerParams(vmem_limit_bytes=8 * MIB),
        name="prepare_other" if other else "prepare_kept",
    )(*streams, *so_far)


def finish_kernel(rank, merged_ref, kept_ref, other_ref, inverse_ref, own_ref, peer_ref, new_hbm, factor_hbm, staged, factor_ref, sems):
    run = kept_ref.shape[0]
    kept = kept_half()
    raw = own_ref[...] + peer_ref[...]
    small = sum(inverse_ref[8 * k : 8 * k + rank, :] * raw[k : k + 1] for k in range(rank))
    factor_ref[...] = small
    copies = [pltpu.make_async_copy(factor_ref, factor_hbm, sems.at[0])]
    copies[0].start()
    weight = sum(inverse_ref[8 * (rank + k) : 8 * (rank + k) + rank, :] * small[k : k + 1] for k in range(rank))
    high, low = split_bf16(weight)
    zero = jnp.zeros((rank, LANES), F32)
    blocks = []
    for fold in range(FOLD):
        parts = [part if u == fold else zero for part in (high, high, low, zero) for u in range(FOLD)]
        blocks.append(jnp.concatenate(parts, axis=0))
    right = jnp.concatenate(blocks, axis=1).astype(BF16)
    for left_ref, half in ((kept_ref, kept), (other_ref, 1 - kept)):
        for start, size in pieces(run // LANES, 4):
            product = jnp.dot(left_ref[start : start + size, :], right, preferred_element_type=F32)
            for fold in range(FOLD):
                at = row_slice(half, fold, run, start, size)
                staged[at, :] = (merged_ref[at, :] - product[:, fold * LANES : (fold + 1) * LANES]).astype(BF16)
                copy = pltpu.make_async_copy(staged.at[at], new_hbm.at[at], sems.at[len(copies)])
                copy.start()
                copies.append(copy)
    for copy in copies:
        copy.wait()


def finish(merged, left_kept, left_other, inverse, own, peer):
    rows, width = merged.shape
    rank = own.shape[0]
    steps = 1 + 2 * FOLD * len(pieces(left_kept.shape[0] // LANES, 4))
    return pl.pallas_call(
        functools.partial(finish_kernel, rank),
        out_shape=(jax.ShapeDtypeStruct((rows, width), BF16), jax.ShapeDtypeStruct((rank, width), F32)),
        in_specs=[VMEM] * 6,
        out_specs=(HBM, HBM),
        scratch_shapes=[
            pltpu.VMEM((rows, width), BF16),
            pltpu.VMEM((rank, width), F32),
            pltpu.SemaphoreType.DMA((steps,)),
        ],
        compiler_params=pltpu.CompilerParams(vmem_limit_bytes=8 * MIB),
        name="finish",
    )(merged, left_kept, left_other, inverse, own, peer)


def per_device(gradient_part, carried_error, query_basis):
    width = gradient_part.shape[3]
    rows = gradient_part.shape[1] * gradient_part.shape[2]
    rank = query_basis.shape[1]
    heads, replicas = lax.axis_size("head"), lax.axis_size("dp")

    def swap(x, bits):
        return lax.ppermute(x, ("head", "dp"), [(i, i ^ bits) for i in range(heads * replicas)])

    gradient, error, left, *sent = project_sent(
        gradient_part.reshape(rows, width), carried_error.reshape(rows, width), query_basis.T
    )
    mine = project_kept(gradient, error, left)
    partner = replicas
    others = [1 << b for b in range((heads * replicas).bit_length() - 1) if 1 << b != partner]
    kept, other = [], []
    for s in range(STREAMS):
        turn = len(others) * s // STREAMS
        value = mine[s] + swap(sent[s], partner)
        for bit in others[turn:] + others[:turn]:
            value = value + swap(value, bit | partner)
        kept.append(value)
        other.append(swap(value, partner))
    merged = merge(gradient, error)
    own = factor(gradient, error, kept, (), rank)
    left_kept, gram = prepare(kept, (), rows // (2 * FOLD), rank, replicas)
    own = factor(gradient, error, other, (own,), rank)
    left_other, inverse = prepare(other, (gram,), rows // (2 * FOLD), rank, replicas)
    peer = jnp.zeros_like(own)
    total = own
    bit = 1
    while bit < replicas:
        peer = lax.ppermute(total, "dp", [(i, i ^ bit) for i in range(replicas)])
        own, total = total, total + peer
        bit *= 2
    new_error, compressed = finish(merged, left_kept, left_other, inverse, own, peer)
    return new_error.reshape(gradient_part.shape), compressed.T


def solution(mesh):
    in_specs = (P("dp", None, None, "head"), P("dp", None, None, "head"), P("head", None))
    out_specs = (P("dp", None, None, "head"), P("head", None))
    return jax.shard_map(
        per_device, mesh=mesh, in_specs=in_specs, out_specs=out_specs, check_vma=False
    )
```

```python
import functools

import jax
import jax.numpy as jnp
from jax import lax
from jax.experimental import pallas as pl
from jax.experimental.pallas import tpu as pltpu
from jax.sharding import PartitionSpec as P

STREAMS = 1
FOLD = 2
LANES = 128
MIB = 1 << 20
BF16, F32 = jnp.bfloat16, jnp.float32
VMEM = pl.BlockSpec(memory_space=pltpu.VMEM)
HBM = pl.BlockSpec(memory_space=pltpu.HBM)


def split_bf16(x):
    high = x.astype(BF16).astype(F32)
    return high, (x - high).astype(BF16).astype(F32)


def pieces(total, most):
    count = -(-total // most)
    ends = [total * i // count for i in range(count + 1)]
    return [(a * LANES, (b - a) * LANES) for a, b in zip(ends, ends[1:])]


def stream_pieces(run):
    tiles = run // LANES
    ends = [-(-tiles * i // STREAMS) for i in range(STREAMS + 1)]
    return [(a * LANES, (b - a) * LANES) for a, b in zip(ends, ends[1:])]


def kept_half():
    parity = 0
    for axis in ("head", "dp"):
        place = lax.axis_index(axis)
        for bit in range(lax.axis_size(axis).bit_length() - 1):
            parity = parity + lax.rem(place // (1 << bit), 2)
    return lax.rem(parity, 2)


def row_slice(half, fold, run, start, size):
    return pl.ds(pl.multiple_of(half * (FOLD * run) + (fold * run + start), LANES), size)


def project_half(half, left_ref, g_ref, e_ref, outs, ready):
    run = g_ref.shape[0] // (2 * FOLD)
    rows = left_ref.shape[0] // FOLD
    for fold in range(FOLD):
        ready(fold)
        at = row_slice(half, fold, run, 0, run)
        both = jnp.concatenate([g_ref[at, :], e_ref[at, :]], axis=1)
        left = left_ref[fold * rows : (fold + 1) * rows, :]
        product = lax.dot_general(left, both, (((1,), (1,)), ((), ())), preferred_element_type=F32)
        total = product[: rows // 2] + product[rows // 2 :]
        for out, (start, size) in zip(outs, stream_pieces(run)):
            part = total[:, start : start + size]
            out[...] = part if fold == 0 else out[...] + part


def project_sent_kernel(rank, g_hbm, e_hbm, q_hbm, g_ref, e_ref, left_ref, *rest):
    outs, (q_ref, sems, q_sem) = rest[:STREAMS], rest[STREAMS:]
    run = g_ref.shape[0] // (2 * FOLD)
    kept = kept_half()
    query_copy = pltpu.make_async_copy(q_hbm, q_ref, q_sem)
    query_copy.start()
    copies = []
    for part, half in enumerate((1 - kept, kept)):
        for fold in range(FOLD):
            at, n = row_slice(half, fold, run, 0, run), len(copies)
            pair = (
                pltpu.make_async_copy(g_hbm.at[at], g_ref.at[at], sems.at[0, n]),
                pltpu.make_async_copy(e_hbm.at[at], e_ref.at[at], sems.at[1, n]),
            )
            for copy in pair:
                copy.start()
            copies.append(pair)
    query_copy.wait()
    high, low = split_bf16(q_ref[...])
    zero = jnp.zeros((rank, LANES), F32)
    for fold in range(FOLD):
        parts = [part if u == fold else zero for part in (high, low) for u in range(FOLD)]
        part = jnp.concatenate(parts, axis=0).astype(BF16)
        rows = part.shape[0]
        left_ref[fold * rows : (fold + 1) * rows, :] = jnp.concatenate([part, part], axis=1)

    def ready(n):
        for copy in copies[n]:
            copy.wait()

    project_half(1 - kept, left_ref, g_ref, e_ref, outs, ready)
    for fold in range(FOLD):
        ready(FOLD + fold)


def project_sent(gradient, error, query_t):
    rows, width = gradient.shape
    rank = query_t.shape[0]
    parts = tuple(pltpu.VMEM((FOLD * rank, w), F32) for _, w in stream_pieces(rows // (2 * FOLD)))
    return pl.pallas_call(
        functools.partial(project_sent_kernel, rank),
        out_shape=(pltpu.VMEM((rows, width), BF16),) * 2 + (pltpu.VMEM((FOLD * 2 * FOLD * rank, 2 * width), BF16),) + parts,
        in_specs=[HBM] * 3,
        out_specs=(VMEM,) * (3 + STREAMS),
        scratch_shapes=[
            pltpu.VMEM((rank, width), F32),
            pltpu.SemaphoreType.DMA((2, 2 * FOLD)),
            pltpu.SemaphoreType.DMA,
        ],
        compiler_params=pltpu.CompilerParams(vmem_limit_bytes=4 * MIB),
        name="project_sent",
    )(*(pltpu.with_memory_space_constraint(x, pltpu.HBM) for x in (gradient, error, query_t)))


def project_kept_kernel(g_ref, e_ref, left_ref, *outs):
    project_half(kept_half(), left_ref, g_ref, e_ref, outs, lambda fold: None)


def project_kept(gradient, error, left):
    rows = left.shape[0] // FOLD
    parts = tuple(pltpu.VMEM((rows // 2, w), F32) for _, w in stream_pieces(gradient.shape[0] // (2 * FOLD)))
    return pl.pallas_call(
        project_kept_kernel,
        out_shape=parts,
        in_specs=[VMEM] * 3,
        out_specs=(VMEM,) * STREAMS,
        compiler_params=pltpu.CompilerParams(vmem_limit_bytes=4 * MIB),
        name="project_kept",
    )(gradient, error, left)


def merge_kernel(g_ref, e_ref, out_ref):
    def step(i, _):
        at = pl.ds(pl.multiple_of(i * LANES, LANES), LANES)
        out_ref[at, :] = g_ref[at, :].astype(F32) + e_ref[at, :].astype(F32)
        return 0

    lax.fori_loop(0, g_ref.shape[0] // LANES, step, 0, unroll=2)


def merge(gradient, error):
    return pl.pallas_call(
        merge_kernel,
        out_shape=pltpu.VMEM(gradient.shape, F32),
        in_specs=[VMEM] * 2,
        out_specs=VMEM,
        compiler_params=pltpu.CompilerParams(vmem_limit_bytes=4 * MIB),
        name="merge",
    )(gradient, error)


def factor_kernel(rank, other, g_ref, e_ref, *rest):
    streams, so_far, (out_ref,) = rest[:STREAMS], rest[STREAMS:-1], rest[-1:]
    run = g_ref.shape[0] // (2 * FOLD)
    kept = kept_half()
    half = 1 - kept if other else kept
    sums = [jnp.zeros((2 * FOLD * rank, 2 * LANES), F32) for _ in range(FOLD)]
    for s, (base, width) in enumerate(stream_pieces(run)):
        for start, size in pieces(width // LANES, 7):
            left = jnp.concatenate(split_bf16(streams[s][:, start : start + size]), axis=0).astype(BF16)
            for fold in range(FOLD):
                at = row_slice(half, fold, run, base + start, size)
                both = jnp.concatenate([g_ref[at, :], e_ref[at, :]], axis=1)
                sums[fold] += jnp.dot(left, both, preferred_element_type=F32)
    total = so_far[0][...] if so_far else jnp.zeros((rank, LANES), F32)
    for fold in range(FOLD):
        whole = sums[fold][:, :LANES] + sums[fold][:, LANES:]
        whole = whole[: FOLD * rank] + whole[FOLD * rank :]
        total += whole[fold * rank : (fold + 1) * rank]
    out_ref[...] = total


def factor(gradient, error, streams, so_far, rank):
    width = gradient.shape[1]
    other = len(so_far) > 0
    return pl.pallas_call(
        functools.partial(factor_kernel, rank, other),
        out_shape=pltpu.VMEM((rank, width), F32),
        in_specs=[VMEM] * (2 + STREAMS + len(so_far)),
        out_specs=VMEM,
        compiler_params=pltpu.CompilerParams(vmem_limit_bytes=4 * MIB),
        name="factor_other" if other else "factor_kept",
    )(gradient, error, *streams, *so_far)


def solve(rank, replicas, gram, out_ref):
    lower, reciprocal = {}, {}
    for j in range(rank):
        for i in range(j, rank):
            value = gram(i, j)
            for k in range(j):
                value = value - lower[i, k] * lower[j, k]
            if i == j:
                reciprocal[j] = 1.0 / jnp.sqrt(value)
            else:
                lower[i, j] = value * reciprocal[j]
    inverse = {}
    for j in range(rank):
        inverse[j, j] = reciprocal[j]
        for i in range(j + 1, rank):
            value = lower[i, j] * inverse[j, j]
            for k in range(j + 1, i):
                value = value + lower[i, k] * inverse[k, j]
            inverse[i, j] = -value * reciprocal[i]
    zero = jnp.zeros((1, LANES), F32)
    for k in range(rank):
        for j in range(rank):
            column = inverse[j, k] * (1.0 / replicas) if j >= k else zero
            row = inverse[k, j] if k >= j else zero
            out_ref[8 * k + j : 8 * k + j + 1, :] = column
            out_ref[8 * (rank + k) + j : 8 * (rank + k) + j + 1, :] = row


def prepare_kernel(rank, replicas, other, *rest):
    streams, so_far, (left_ref, out_ref) = rest[:STREAMS], rest[STREAMS:-2], rest[-2:]
    rows = FOLD * rank
    run = left_ref.shape[0]
    grams = [jnp.zeros((rows, LANES), F32) for _ in range(rank)]
    for s, (base, width) in enumerate(stream_pieces(run)):
        for start, size in pieces(width // LANES, 7):
            part = streams[s][:, start : start + size]
            high, low = split_bf16(part)
            left = jnp.concatenate([high, low, high, jnp.zeros_like(part)], axis=0)
            left_ref[base + start : base + start + size, :] = left.T.astype(BF16)
            for d in range(rank):
                product = part * (part if d == 0 else pltpu.roll(part, d, 0))
                for c in range(0, size, LANES):
                    grams[d] += product[:, c : c + LANES]
    sums = []
    for d in range(rank):
        value = jnp.broadcast_to(jnp.sum(grams[d], axis=1, keepdims=True), (rows, LANES))
        sums.append(value + so_far[0][d * rows : (d + 1) * rows, :] if so_far else value)
    if not other:
        for d in range(rank):
            out_ref[d * rows : (d + 1) * rows, :] = sums[d]
        return

    def gram(i, j):
        return sum(sums[i - j][fold * rank + i : fold * rank + i + 1] for fold in range(FOLD))

    solve(rank, replicas, gram, out_ref)


def prepare(streams, so_far, run, rank, replicas):
    other = len(so_far) > 0
    out_rows = 16 * rank if other else rank * FOLD * rank
    return pl.pallas_call(
        functools.partial(prepare_kernel, rank, replicas, other),
        out_shape=(pltpu.VMEM((run, 4 * FOLD * rank), BF16), pltpu.VMEM((out_rows, LANES), F32)),
        in_specs=[VMEM] * (STREAMS + len(so_far)),
        out_specs=(VMEM,) * 2,
        compiler_params=pltpu.CompilerParams(vmem_limit_bytes=8 * MIB),
        name="prepare_other" if other else "prepare_kept",
    )(*streams, *so_far)


def finish_kernel(rank, merged_ref, kept_ref, other_ref, inverse_ref, own_ref, peer_ref, new_hbm, factor_hbm, staged, factor_ref, sems):
    run = kept_ref.shape[0]
    kept = kept_half()
    raw = own_ref[...] + peer_ref[...]
    small = sum(inverse_ref[8 * k : 8 * k + rank, :] * raw[k : k + 1] for k in range(rank))
    factor_ref[...] = small
    copies = [pltpu.make_async_copy(factor_ref, factor_hbm, sems.at[0])]
    copies[0].start()
    weight = sum(inverse_ref[8 * (rank + k) : 8 * (rank + k) + rank, :] * small[k : k + 1] for k in range(rank))
    high, low = split_bf16(weight)
    zero = jnp.zeros((rank, LANES), F32)
    blocks = []
    for fold in range(FOLD):
        parts = [part if u == fold else zero for part in (high, high, low, zero) for u in range(FOLD)]
        blocks.append(jnp.concatenate(parts, axis=0))
    right = jnp.concatenate(blocks, axis=1).astype(BF16)
    for left_ref, half in ((kept_ref, kept), (other_ref, 1 - kept)):
        for start, size in pieces(run // LANES, 4):
            product = jnp.dot(left_ref[start : start + size, :], right, preferred_element_type=F32)
            for fold in range(FOLD):
                at = row_slice(half, fold, run, start, size)
                staged[at, :] = (merged_ref[at, :] - product[:, fold * LANES : (fold + 1) * LANES]).astype(BF16)
                copy = pltpu.make_async_copy(staged.at[at], new_hbm.at[at], sems.at[len(copies)])
                copy.start()
                copies.append(copy)
    for copy in copies:
        copy.wait()


def finish(merged, left_kept, left_other, inverse, own, peer):
    rows, width = merged.shape
    rank = own.shape[0]
    steps = 1 + 2 * FOLD * len(pieces(left_kept.shape[0] // LANES, 4))
    return pl.pallas_call(
        functools.partial(finish_kernel, rank),
        out_shape=(jax.ShapeDtypeStruct((rows, width), BF16), jax.ShapeDtypeStruct((rank, width), F32)),
        in_specs=[VMEM] * 6,
        out_specs=(HBM, HBM),
        scratch_shapes=[
            pltpu.VMEM((rows, width), BF16),
            pltpu.VMEM((rank, width), F32),
            pltpu.SemaphoreType.DMA((steps,)),
        ],
        compiler_params=pltpu.CompilerParams(vmem_limit_bytes=8 * MIB),
        name="finish",
    )(merged, left_kept, left_other, inverse, own, peer)


def sum_over(value, bits, partner, swap):
    term = value.astype(BF16)
    near = swap(term, bits[0] | partner)
    if len(bits) == 1:
        return term.astype(F32) + near.astype(F32)
    across = swap(term, bits[0] ^ bits[1])
    far = swap(term, bits[1] | partner)
    return (term.astype(F32) + near.astype(F32)) + (far.astype(F32) + across.astype(F32))


def per_device(gradient_part, carried_error, query_basis):
    width = gradient_part.shape[3]
    rows = gradient_part.shape[1] * gradient_part.shape[2]
    rank = query_basis.shape[1]
    heads, replicas = lax.axis_size("head"), lax.axis_size("dp")

    def swap(x, bits):
        return lax.ppermute(x, ("head", "dp"), [(i, i ^ bits) for i in range(heads * replicas)])

    gradient, error, left, *sent = project_sent(
        gradient_part.reshape(rows, width), carried_error.reshape(rows, width), query_basis.T
    )
    mine = project_kept(gradient, error, left)
    partner = replicas
    others = [1 << b for b in range((heads * replicas).bit_length() - 1) if 1 << b != partner]
    kept, other = [], []
    for s in range(STREAMS):
        value = mine[s] + swap(sent[s], partner)
        for first in range(0, len(others), 2):
            value = sum_over(value, others[first : first + 2], partner, swap)
        kept.append(value)
        other.append(swap(value, partner))
    merged = merge(gradient, error)
    own = factor(gradient, error, kept, (), rank)
    left_kept, gram = prepare(kept, (), rows // (2 * FOLD), rank, replicas)
    own = factor(gradient, error, other, (own,), rank)
    left_other, inverse = prepare(other, (gram,), rows // (2 * FOLD), rank, replicas)
    peer = jnp.zeros_like(own)
    total = own
    bit = 1
    while bit < replicas:
        peer = lax.ppermute(total, "dp", [(i, i ^ bit) for i in range(replicas)])
        own, total = total, total + peer
        bit *= 2
    new_error, compressed = finish(merged, left_kept, left_other, inverse, own, peer)
    return new_error.reshape(gradient_part.shape), compressed.T


def solution(mesh):
    in_specs = (P("dp", None, None, "head"), P("dp", None, None, "head"), P("head", None))
    out_specs = (P("dp", None, None, "head"), P("head", None))
    return jax.shard_map(
        per_device, mesh=mesh, in_specs=in_specs, out_specs=out_specs, check_vma=False
    )
```

```python
import functools

import jax
import jax.numpy as jnp
from jax import lax
from jax.experimental import pallas as pl
from jax.experimental.pallas import tpu as pltpu
from jax.sharding import PartitionSpec as P


STREAMS = 1
FOLD = 2
LANES = 128
MIB = 1 << 20
BF16, F32 = jnp.bfloat16, jnp.float32
VMEM = pl.BlockSpec(memory_space=pltpu.VMEM)
HBM = pl.BlockSpec(memory_space=pltpu.HBM)


def split_bf16(x):
    high = x.astype(BF16).astype(F32)
    return high, (x - high).astype(BF16).astype(F32)


def pieces(total, most):
    count = -(-total // most)
    ends = [total * i // count for i in range(count + 1)]
    return [(a * LANES, (b - a) * LANES) for a, b in zip(ends, ends[1:])]


def stream_pieces(run):
    tiles = run // LANES
    ends = [-(-tiles * i // STREAMS) for i in range(STREAMS + 1)]
    return [(a * LANES, (b - a) * LANES) for a, b in zip(ends, ends[1:])]


def kept_half():
    parity = 0
    for axis in ("head", "dp"):
        place = lax.axis_index(axis)
        for bit in range(lax.axis_size(axis).bit_length() - 1):
            parity = parity + lax.rem(place // (1 << bit), 2)
    return lax.rem(parity, 2)


def row_slice(half, fold, run, start, size):
    return pl.ds(pl.multiple_of(half * (FOLD * run) + (fold * run + start), LANES), size)


def product_of(half, fold, start, size, left_ref, g_ref, e_ref):
    run = g_ref.shape[0] // (2 * FOLD)
    rows = left_ref.shape[0] // FOLD
    at = row_slice(half, fold, run, start, size)
    both = jnp.concatenate([g_ref[at, :], e_ref[at, :]], axis=1)
    left = left_ref[fold * rows : (fold + 1) * rows, :]
    product = lax.dot_general(left, both, (((1,), (1,)), ((), ())), preferred_element_type=F32)
    return product[: rows // 2] + product[rows // 2 :]


def early_columns(run):
    return LANES * (run // LANES * 4 // 9)


def project_sent_kernel(rank, g_hbm, e_hbm, q_hbm, g_ref, e_ref, left_ref, *rest):
    sent_ref, early_ref, q_ref, sems, q_sem = rest
    run = g_ref.shape[0] // (2 * FOLD)
    kept = kept_half()
    query_copy = pltpu.make_async_copy(q_hbm, q_ref, q_sem)
    query_copy.start()
    copies = []
    for part, half in enumerate((1 - kept, kept)):
        for fold in range(FOLD):
            at, n = row_slice(half, fold, run, 0, run), len(copies)
            pair = (
                pltpu.make_async_copy(g_hbm.at[at], g_ref.at[at], sems.at[0, n]),
                pltpu.make_async_copy(e_hbm.at[at], e_ref.at[at], sems.at[1, n]),
            )
            for copy in pair:
                copy.start()
            copies.append(pair)
    query_copy.wait()
    high, low = split_bf16(q_ref[...])
    zero = jnp.zeros((rank, LANES), F32)
    for fold in range(FOLD):
        parts = [part if u == fold else zero for part in (high, low) for u in range(FOLD)]
        part = jnp.concatenate(parts, axis=0).astype(BF16)
        rows = part.shape[0]
        left_ref[fold * rows : (fold + 1) * rows, :] = jnp.concatenate([part, part], axis=1)

    def ready(n):
        for copy in copies[n]:
            copy.wait()

    for fold in range(FOLD):
        ready(fold)
        part = product_of(1 - kept, fold, 0, run, left_ref, g_ref, e_ref)
        sent_ref[...] = part if fold == 0 else sent_ref[...] + part
    ready(FOLD)
    early_ref[...] = product_of(kept, 0, 0, early_ref.shape[1], left_ref, g_ref, e_ref)
    for fold in range(1, FOLD):
        ready(FOLD + fold)


def project_sent(gradient, error, query_t):
    rows, width = gradient.shape
    rank = query_t.shape[0]
    run = rows // (2 * FOLD)
    parts = tuple(pltpu.VMEM((FOLD * rank, w), F32) for w in (run, early_columns(run)))
    return pl.pallas_call(
        functools.partial(project_sent_kernel, rank),
        out_shape=(pltpu.VMEM((rows, width), BF16),) * 2 + (pltpu.VMEM((FOLD * 2 * FOLD * rank, 2 * width), BF16),) + parts,
        in_specs=[HBM] * 3,
        out_specs=(VMEM,) * 5,
        scratch_shapes=[
            pltpu.VMEM((rank, width), F32),
            pltpu.SemaphoreType.DMA((2, 2 * FOLD)),
            pltpu.SemaphoreType.DMA,
        ],
        compiler_params=pltpu.CompilerParams(vmem_limit_bytes=4 * MIB),
        name="project_sent",
    )(*(pltpu.with_memory_space_constraint(x, pltpu.HBM) for x in (gradient, error, query_t)))


def project_kept_kernel(g_ref, e_ref, left_ref, early_ref, out_ref):
    kept = kept_half()
    early, run = early_ref.shape[1], out_ref.shape[1]
    out_ref[:, :early] = early_ref[...]
    out_ref[:, early:] = product_of(kept, 0, early, run - early, left_ref, g_ref, e_ref)
    for fold in range(1, FOLD):
        out_ref[...] += product_of(kept, fold, 0, run, left_ref, g_ref, e_ref)


def project_kept(gradient, error, left, early):
    return pl.pallas_call(
        project_kept_kernel,
        out_shape=pltpu.VMEM((early.shape[0], gradient.shape[0] // (2 * FOLD)), F32),
        in_specs=[VMEM] * 4,
        out_specs=VMEM,
        compiler_params=pltpu.CompilerParams(vmem_limit_bytes=4 * MIB),
        name="project_kept",
    )(gradient, error, left, early)


def merge_kernel(g_ref, e_ref, out_ref, rounded_ref):
    def step(i, _):
        at = pl.ds(pl.multiple_of(i * LANES, LANES), LANES)
        total = g_ref[at, :].astype(F32) + e_ref[at, :].astype(F32)
        out_ref[at, :] = total
        rounded_ref[at, :] = total.astype(BF16)
        return 0

    lax.fori_loop(0, g_ref.shape[0] // LANES, step, 0, unroll=2)


def merge(gradient, error):
    return pl.pallas_call(
        merge_kernel,
        out_shape=(pltpu.VMEM(gradient.shape, F32), pltpu.VMEM(gradient.shape, BF16)),
        in_specs=[VMEM] * 2,
        out_specs=(VMEM,) * 2,
        compiler_params=pltpu.CompilerParams(vmem_limit_bytes=4 * MIB),
        name="merge",
    )(gradient, error)


def factor_kernel(rank, other, merged_ref, *rest):
    streams, so_far, (out_ref,) = rest[:STREAMS], rest[STREAMS:-1], rest[-1:]
    run = merged_ref.shape[0] // (2 * FOLD)
    kept = kept_half()
    half = 1 - kept if other else kept
    sums = jnp.zeros((2 * FOLD * rank, FOLD * LANES), F32)
    for s, (base, width) in enumerate(stream_pieces(run)):
        for start, size in pieces(width // LANES, 7):
            left = jnp.concatenate(split_bf16(streams[s][:, start : start + size]), axis=0).astype(BF16)
            folds = [merged_ref[row_slice(half, fold, run, base + start, size), :] for fold in range(FOLD)]
            sums += jnp.dot(left, jnp.concatenate(folds, axis=1), preferred_element_type=F32)
    total = so_far[0][...] if so_far else jnp.zeros((rank, LANES), F32)
    sums = sums[: FOLD * rank] + sums[FOLD * rank :]
    for fold in range(FOLD):
        total += sums[fold * rank : (fold + 1) * rank, fold * LANES : (fold + 1) * LANES]
    out_ref[...] = total


def factor(rounded, streams, so_far, rank):
    width = rounded.shape[1]
    other = len(so_far) > 0
    return pl.pallas_call(
        functools.partial(factor_kernel, rank, other),
        out_shape=pltpu.VMEM((rank, width), F32),
        in_specs=[VMEM] * (1 + STREAMS + len(so_far)),
        out_specs=VMEM,
        compiler_params=pltpu.CompilerParams(vmem_limit_bytes=4 * MIB),
        name="factor_other" if other else "factor_kept",
    )(rounded, *streams, *so_far)


def solve(rank, replicas, gram, out_ref):
    lower, reciprocal = {}, {}
    for j in range(rank):
        for i in range(j, rank):
            value = gram(i, j)
            for k in range(j):
                value = value - lower[i, k] * lower[j, k]
            if i == j:
                reciprocal[j] = 1.0 / jnp.sqrt(value)
            else:
                lower[i, j] = value * reciprocal[j]
    inverse = {}
    for j in range(rank):
        inverse[j, j] = reciprocal[j]
        for i in range(j + 1, rank):
            value = lower[i, j] * inverse[j, j]
            for k in range(j + 1, i):
                value = value + lower[i, k] * inverse[k, j]
            inverse[i, j] = -value * reciprocal[i]
    zero = jnp.zeros((1, LANES), F32)
    for k in range(rank):
        for j in range(rank):
            column = inverse[j, k] * (1.0 / replicas) if j >= k else zero
            row = inverse[k, j] if k >= j else zero
            out_ref[8 * k + j : 8 * k + j + 1, :] = column
            out_ref[8 * (rank + k) + j : 8 * (rank + k) + j + 1, :] = row


def prepare_kernel(rank, replicas, other, *rest):
    streams, so_far, (left_ref, out_ref) = rest[:STREAMS], rest[STREAMS:-2], rest[-2:]
    rows = FOLD * rank
    run = left_ref.shape[0]
    grams = [jnp.zeros((rows, LANES), F32) for _ in range(rank)]
    for s, (base, width) in enumerate(stream_pieces(run)):
        for start, size in pieces(width // LANES, 7):
            part = streams[s][:, start : start + size]
            high, low = split_bf16(part)
            left = jnp.concatenate([high, low, high, jnp.zeros_like(part)], axis=0)
            left_ref[base + start : base + start + size, :] = left.T.astype(BF16)
            for d in range(rank):
                product = part * (part if d == 0 else pltpu.roll(part, d, 0))
                for c in range(0, size, LANES):
                    grams[d] += product[:, c : c + LANES]
    sums = []
    for d in range(rank):
        value = jnp.broadcast_to(jnp.sum(grams[d], axis=1, keepdims=True), (rows, LANES))
        sums.append(value + so_far[0][d * rows : (d + 1) * rows, :] if so_far else value)
    if not other:
        for d in range(rank):
            out_ref[d * rows : (d + 1) * rows, :] = sums[d]
        return

    def gram(i, j):
        return sum(sums[i - j][fold * rank + i : fold * rank + i + 1] for fold in range(FOLD))

    solve(rank, replicas, gram, out_ref)


def prepare(streams, so_far, run, rank, replicas):
    other = len(so_far) > 0
    out_rows = 16 * rank if other else rank * FOLD * rank
    return pl.pallas_call(
        functools.partial(prepare_kernel, rank, replicas, other),
        out_shape=(pltpu.VMEM((run, 4 * FOLD * rank), BF16), pltpu.VMEM((out_rows, LANES), F32)),
        in_specs=[VMEM] * (STREAMS + len(so_far)),
        out_specs=(VMEM,) * 2,
        compiler_params=pltpu.CompilerParams(vmem_limit_bytes=8 * MIB),
        name="prepare_other" if other else "prepare_kept",
    )(*streams, *so_far)


def finish_kernel(rank, merged_ref, kept_ref, other_ref, inverse_ref, own_ref, peer_ref, new_hbm, factor_hbm, staged, factor_ref, sems):
    run = kept_ref.shape[0]
    kept = kept_half()
    raw = own_ref[...] + peer_ref[...]
    small = sum(inverse_ref[8 * k : 8 * k + rank, :] * raw[k : k + 1] for k in range(rank))
    factor_ref[...] = small
    copies = [pltpu.make_async_copy(factor_ref, factor_hbm, sems.at[0])]
    copies[0].start()
    weight = sum(inverse_ref[8 * (rank + k) : 8 * (rank + k) + rank, :] * small[k : k + 1] for k in range(rank))
    high, low = split_bf16(weight)
    zero = jnp.zeros((rank, LANES), F32)
    right = []
    for fold in range(FOLD):
        parts = [part if u == fold else zero for part in (high, high, low, zero) for u in range(FOLD)]
        right.append(jnp.concatenate(parts, axis=0).astype(BF16))
    for left_ref, half in ((kept_ref, kept), (other_ref, 1 - kept)):
        for start, size in pieces(run // LANES, 7):
            for fold in range(FOLD):
                at = row_slice(half, fold, run, start, size)
                product = jnp.dot(left_ref[start : start + size, :], right[fold], preferred_element_type=F32)
                staged[at, :] = (merged_ref[at, :] - product).astype(BF16)
                copy = pltpu.make_async_copy(staged.at[at], new_hbm.at[at], sems.at[len(copies)])
                copy.start()
                copies.append(copy)
    for copy in copies:
        copy.wait()


def finish(merged, left_kept, left_other, inverse, own, peer):
    rows, width = merged.shape
    rank = own.shape[0]
    steps = 1 + 2 * FOLD * len(pieces(left_kept.shape[0] // LANES, 7))
    return pl.pallas_call(
        functools.partial(finish_kernel, rank),
        out_shape=(jax.ShapeDtypeStruct((rows, width), BF16), jax.ShapeDtypeStruct((rank, width), F32)),
        in_specs=[VMEM] * 6,
        out_specs=(HBM, HBM),
        scratch_shapes=[
            pltpu.VMEM((rows, width), BF16),
            pltpu.VMEM((rank, width), F32),
            pltpu.SemaphoreType.DMA((steps,)),
        ],
        compiler_params=pltpu.CompilerParams(vmem_limit_bytes=8 * MIB),
        name="finish",
    )(merged, left_kept, left_other, inverse, own, peer)


def sum_over(value, bits, partner, swap):
    term = value.astype(BF16)
    near = swap(term, bits[0] | partner)
    if len(bits) == 1:
        return term.astype(F32) + near.astype(F32)
    across = swap(term, bits[0] ^ bits[1])
    far = swap(term, bits[1] | partner)
    return (term.astype(F32) + near.astype(F32)) + (far.astype(F32) + across.astype(F32))


def chip_bits(heads, replicas):
    bits = [1 << b for b in range((heads * replicas).bit_length() - 1) if 1 << b != replicas]
    return [bits[i : i + 2] for i in range(0, len(bits), 2)]


def per_device(gradient_part, carried_error, query_basis):
    width = gradient_part.shape[3]
    rows = gradient_part.shape[1] * gradient_part.shape[2]
    rank = query_basis.shape[1]
    heads, replicas = lax.axis_size("head"), lax.axis_size("dp")

    def swap(x, bits):
        return lax.ppermute(x, ("head", "dp"), [(i, i ^ bits) for i in range(heads * replicas)])

    gradient, error, left, sent, early = project_sent(
        gradient_part.reshape(rows, width), carried_error.reshape(rows, width), query_basis.T
    )
    mine = project_kept(gradient, error, left, early)
    partner = replicas
    value = mine + swap(sent, partner)
    for bits in chip_bits(heads, replicas):
        value = sum_over(value, bits, partner, swap)
    kept, other = [value], [swap(value, partner)]
    merged, rounded = merge(gradient, error)
    own = factor(rounded, kept, (), rank)
    left_kept, gram = prepare(kept, (), rows // (2 * FOLD), rank, replicas)
    own = factor(rounded, other, (own,), rank)
    left_other, inverse = prepare(other, (gram,), rows // (2 * FOLD), rank, replicas)
    peer = jnp.zeros_like(own)
    total = own
    bit = 1
    while bit < replicas:
        peer = lax.ppermute(total, "dp", [(i, i ^ bit) for i in range(replicas)])
        own, total = total, total + peer
        bit *= 2
    new_error, compressed = finish(merged, left_kept, left_other, inverse, own, peer)
    return new_error.reshape(gradient_part.shape), compressed.T


def solution(mesh):
    in_specs = (P("dp", None, None, "head"), P("dp", None, None, "head"), P("head", None))
    out_specs = (P("dp", None, None, "head"), P("head", None))

    return jax.shard_map(per_device, mesh=mesh, in_specs=in_specs, out_specs=out_specs, check_vma=False)
```

```python
import functools

import jax
import jax.numpy as jnp
from jax import lax
from jax.experimental import pallas as pl
from jax.experimental.pallas import tpu as pltpu
from jax.sharding import PartitionSpec as P


STREAMS = 1
FOLD = 2
LANES = 128
MIB = 1 << 20
BF16, F32 = jnp.bfloat16, jnp.float32
VMEM = pl.BlockSpec(memory_space=pltpu.VMEM)
HBM = pl.BlockSpec(memory_space=pltpu.HBM)


def split_bf16(x):
    high = x.astype(BF16).astype(F32)
    return high, (x - high).astype(BF16).astype(F32)


def pieces(total, most):
    count = -(-total // most)
    ends = [total * i // count for i in range(count + 1)]
    return [(a * LANES, (b - a) * LANES) for a, b in zip(ends, ends[1:])]


def stream_pieces(run):
    tiles = run // LANES
    ends = [-(-tiles * i // STREAMS) for i in range(STREAMS + 1)]
    return [(a * LANES, (b - a) * LANES) for a, b in zip(ends, ends[1:])]


def chip_bits(heads, replicas):
    bits = [1 << b for b in range((heads * replicas).bit_length() - 1) if 1 << b != replicas]
    return [bits[i : i + 2] for i in range(0, len(bits), 2)]


def kept_half():
    heads, replicas = lax.axis_size("head"), lax.axis_size("dp")
    place = lax.axis_index("head") * replicas + lax.axis_index("dp")
    parity = lax.rem(place // replicas, 2)
    for bits in chip_bits(heads, replicas):
        parity = parity + lax.rem(place // bits[0], 2)
    return lax.rem(parity, 2)


def row_slice(half, fold, run, start, size):
    return pl.ds(pl.multiple_of(half * (FOLD * run) + (fold * run + start), LANES), size)


def product_of(half, fold, start, size, left_ref, g_ref, e_ref):
    run = g_ref.shape[0] // (2 * FOLD)
    rows = left_ref.shape[0] // FOLD
    at = row_slice(half, fold, run, start, size)
    both = jnp.concatenate([g_ref[at, :], e_ref[at, :]], axis=1)
    left = left_ref[fold * rows : (fold + 1) * rows, :]
    product = lax.dot_general(left, both, (((1,), (1,)), ((), ())), preferred_element_type=F32)
    return product[: rows // 2] + product[rows // 2 :]


def early_columns(run):
    return LANES * (run // LANES * 4 // 9)


def project_sent_kernel(rank, g_hbm, e_hbm, q_hbm, g_ref, e_ref, left_ref, *rest):
    sent_ref, early_ref, q_ref, sems, q_sem = rest
    run = g_ref.shape[0] // (2 * FOLD)
    kept = kept_half()
    query_copy = pltpu.make_async_copy(q_hbm, q_ref, q_sem)
    query_copy.start()
    copies = []
    for part, half in enumerate((1 - kept, kept)):
        for fold in range(FOLD):
            at, n = row_slice(half, fold, run, 0, run), len(copies)
            pair = (
                pltpu.make_async_copy(g_hbm.at[at], g_ref.at[at], sems.at[0, n]),
                pltpu.make_async_copy(e_hbm.at[at], e_ref.at[at], sems.at[1, n]),
            )
            for copy in pair:
                copy.start()
            copies.append(pair)
    query_copy.wait()
    high, low = split_bf16(q_ref[...])
    zero = jnp.zeros((rank, LANES), F32)
    for fold in range(FOLD):
        parts = [part if u == fold else zero for part in (high, low) for u in range(FOLD)]
        part = jnp.concatenate(parts, axis=0).astype(BF16)
        rows = part.shape[0]
        left_ref[fold * rows : (fold + 1) * rows, :] = jnp.concatenate([part, part], axis=1)

    def ready(n):
        for copy in copies[n]:
            copy.wait()

    for fold in range(FOLD):
        ready(fold)
        part = product_of(1 - kept, fold, 0, run, left_ref, g_ref, e_ref)
        sent_ref[...] = part if fold == 0 else sent_ref[...] + part
    ready(FOLD)
    early_ref[...] = product_of(kept, 0, 0, early_ref.shape[1], left_ref, g_ref, e_ref)
    for fold in range(1, FOLD):
        ready(FOLD + fold)


def project_sent(gradient, error, query_t):
    rows, width = gradient.shape
    rank = query_t.shape[0]
    run = rows // (2 * FOLD)
    parts = tuple(pltpu.VMEM((FOLD * rank, w), F32) for w in (run, early_columns(run)))
    return pl.pallas_call(
        functools.partial(project_sent_kernel, rank),
        out_shape=(pltpu.VMEM((rows, width), BF16),) * 2 + (pltpu.VMEM((FOLD * 2 * FOLD * rank, 2 * width), BF16),) + parts,
        in_specs=[HBM] * 3,
        out_specs=(VMEM,) * 5,
        scratch_shapes=[
            pltpu.VMEM((rank, width), F32),
            pltpu.SemaphoreType.DMA((2, 2 * FOLD)),
            pltpu.SemaphoreType.DMA,
        ],
        compiler_params=pltpu.CompilerParams(vmem_limit_bytes=4 * MIB),
        name="project_sent",
    )(*(pltpu.with_memory_space_constraint(x, pltpu.HBM) for x in (gradient, error, query_t)))


def project_kept_kernel(g_ref, e_ref, left_ref, early_ref, out_ref):
    kept = kept_half()
    early, run = early_ref.shape[1], out_ref.shape[1]
    out_ref[:, :early] = early_ref[...]
    out_ref[:, early:] = product_of(kept, 0, early, run - early, left_ref, g_ref, e_ref)
    for fold in range(1, FOLD):
        out_ref[...] += product_of(kept, fold, 0, run, left_ref, g_ref, e_ref)


def project_kept(gradient, error, left, early):
    return pl.pallas_call(
        project_kept_kernel,
        out_shape=pltpu.VMEM((early.shape[0], gradient.shape[0] // (2 * FOLD)), F32),
        in_specs=[VMEM] * 4,
        out_specs=VMEM,
        compiler_params=pltpu.CompilerParams(vmem_limit_bytes=4 * MIB),
        name="project_kept",
    )(gradient, error, left, early)


def merge_kernel(g_ref, e_ref, out_ref, kept_ref, sent_ref):
    rows = kept_ref.shape[0]
    kept = kept_half()
    for rounded_ref, half in ((kept_ref, kept), (sent_ref, 1 - kept)):

        def step(i, _):
            to = pl.ds(pl.multiple_of(i * LANES, LANES), LANES)
            at = pl.ds(pl.multiple_of(half * rows + i * LANES, LANES), LANES)
            total = g_ref[at, :].astype(F32) + e_ref[at, :].astype(F32)
            out_ref[at, :] = total
            rounded_ref[to, :] = total.astype(BF16)
            return 0

        lax.fori_loop(0, rows // LANES, step, 0, unroll=2)


def merge(gradient, error):
    rows, width = gradient.shape
    return pl.pallas_call(
        merge_kernel,
        out_shape=(pltpu.VMEM((rows, width), F32),) + (pltpu.VMEM((rows // 2, width), BF16),) * 2,
        in_specs=[VMEM] * 2,
        out_specs=(VMEM,) * 3,
        compiler_params=pltpu.CompilerParams(vmem_limit_bytes=4 * MIB),
        name="merge",
    )(gradient, error)


def by_core(own, partner):
    odd = lax.rem(lax.axis_index("head"), 2) == 1
    return jnp.where(odd, partner, own), jnp.where(odd, own, partner)


def factor_kernel(rank, own_ref, partner_ref, stream_ref, out_ref):
    run = own_ref.shape[0] // FOLD
    sums = [jnp.zeros((2 * FOLD * rank, 2 * LANES), F32) for _ in range(FOLD)]
    for start, size in pieces(run // LANES, 7):
        left = jnp.concatenate(split_bf16(stream_ref[:, start : start + size]), axis=0).astype(BF16)
        for fold in range(FOLD):
            at = pl.ds(fold * run + start, size)
            both = jnp.concatenate([own_ref[at, :], partner_ref[at, :]], axis=1)
            sums[fold] += jnp.dot(left, both, preferred_element_type=F32)
    total = jnp.zeros((rank, 2 * LANES), F32)
    for fold in range(FOLD):
        whole = sums[fold][: FOLD * rank] + sums[fold][FOLD * rank :]
        total += whole[fold * rank : (fold + 1) * rank]
    out_ref[...] = jnp.concatenate(by_core(total[:, :LANES], total[:, LANES:]), axis=0)


def factor(own, partner, stream, rank):
    return pl.pallas_call(
        functools.partial(factor_kernel, rank),
        out_shape=pltpu.VMEM((2 * rank, own.shape[1]), F32),
        in_specs=[VMEM] * 3,
        out_specs=VMEM,
        compiler_params=pltpu.CompilerParams(vmem_limit_bytes=4 * MIB),
        name="factor",
    )(own, partner, stream)


def solve(rank, replicas, gram, out_ref):
    lower, reciprocal = {}, {}
    for j in range(rank):
        for i in range(j, rank):
            value = gram(i, j)
            for k in range(j):
                value = value - lower[i, k] * lower[j, k]
            if i == j:
                reciprocal[j] = 1.0 / jnp.sqrt(value)
            else:
                lower[i, j] = value * reciprocal[j]
    inverse = {}
    for j in range(rank):
        inverse[j, j] = reciprocal[j]
        for i in range(j + 1, rank):
            value = lower[i, j] * inverse[j, j]
            for k in range(j + 1, i):
                value = value + lower[i, k] * inverse[k, j]
            inverse[i, j] = -value * reciprocal[i]
    zero = jnp.zeros((1, LANES), F32)
    for k in range(rank):
        for j in range(rank):
            column = inverse[j, k] * (1.0 / replicas) if j >= k else zero
            row = inverse[k, j] if k >= j else zero
            out_ref[8 * k + j : 8 * k + j + 1, :] = column
            out_ref[8 * (rank + k) + j : 8 * (rank + k) + j + 1, :] = row


def prepare_kernel(rank, replicas, other, *rest):
    streams, so_far, (left_ref, out_ref) = rest[:STREAMS], rest[STREAMS:-2], rest[-2:]
    rows = FOLD * rank
    run = left_ref.shape[0]
    grams = [jnp.zeros((rows, LANES), F32) for _ in range(rank)]
    for s, (base, width) in enumerate(stream_pieces(run)):
        for start, size in pieces(width // LANES, 7):
            part = streams[s][:, start : start + size]
            high, low = split_bf16(part)
            left = jnp.concatenate([high, low, high, jnp.zeros_like(part)], axis=0)
            left_ref[base + start : base + start + size, :] = left.T.astype(BF16)
            for d in range(rank):
                product = part * (part if d == 0 else pltpu.roll(part, d, 0))
                for c in range(0, size, LANES):
                    grams[d] += product[:, c : c + LANES]
    sums = []
    for d in range(rank):
        value = jnp.broadcast_to(jnp.sum(grams[d], axis=1, keepdims=True), (rows, LANES))
        sums.append(value + so_far[0][d * rows : (d + 1) * rows, :] if so_far else value)
    if not other:
        for d in range(rank):
            out_ref[d * rows : (d + 1) * rows, :] = sums[d]
        return

    def gram(i, j):
        return sum(sums[i - j][fold * rank + i : fold * rank + i + 1] for fold in range(FOLD))

    solve(rank, replicas, gram, out_ref)


def prepare(streams, so_far, run, rank, replicas):
    other = len(so_far) > 0
    out_rows = 16 * rank if other else rank * FOLD * rank
    return pl.pallas_call(
        functools.partial(prepare_kernel, rank, replicas, other),
        out_shape=(pltpu.VMEM((run, 4 * FOLD * rank), BF16), pltpu.VMEM((out_rows, LANES), F32)),
        in_specs=[VMEM] * (STREAMS + len(so_far)),
        out_specs=(VMEM,) * 2,
        compiler_params=pltpu.CompilerParams(vmem_limit_bytes=8 * MIB),
        name="prepare_other" if other else "prepare_kept",
    )(*streams, *so_far)


def finish_kernel(rank, merged_ref, kept_ref, other_ref, inverse_ref, one_ref, two_ref, new_hbm, factor_hbm, staged, factor_ref, sems):
    run = kept_ref.shape[0]
    kept = kept_half()
    raw = one_ref[...] + two_ref[...]
    raw, _ = by_core(raw[:rank], raw[rank:])
    small = sum(inverse_ref[8 * k : 8 * k + rank, :] * raw[k : k + 1] for k in range(rank))
    factor_ref[...] = small
    copies = [pltpu.make_async_copy(factor_ref, factor_hbm, sems.at[0])]
    copies[0].start()
    weight = sum(inverse_ref[8 * (rank + k) : 8 * (rank + k) + rank, :] * small[k : k + 1] for k in range(rank))
    high, low = split_bf16(weight)
    zero = jnp.zeros((rank, LANES), F32)
    right = []
    for fold in range(FOLD):
        parts = [part if u == fold else zero for part in (high, high, low, zero) for u in range(FOLD)]
        right.append(jnp.concatenate(parts, axis=0).astype(BF16))
    for left_ref, half in ((kept_ref, kept), (other_ref, 1 - kept)):
        for start, size in pieces(run // LANES, 7):
            for fold in range(FOLD):
                at = row_slice(half, fold, run, start, size)
                product = jnp.dot(left_ref[start : start + size, :], right[fold], preferred_element_type=F32)
                staged[at, :] = (merged_ref[at, :] - product).astype(BF16)
                copy = pltpu.make_async_copy(staged.at[at], new_hbm.at[at], sems.at[len(copies)])
                copy.start()
                copies.append(copy)
    for copy in copies:
        copy.wait()


def finish(merged, left_kept, left_other, inverse, one, two):
    rows, width = merged.shape
    rank = one.shape[0] // 2
    steps = 1 + 2 * FOLD * len(pieces(left_kept.shape[0] // LANES, 7))
    return pl.pallas_call(
        functools.partial(finish_kernel, rank),
        out_shape=(jax.ShapeDtypeStruct((rows, width), BF16), jax.ShapeDtypeStruct((rank, width), F32)),
        in_specs=[VMEM] * 6,
        out_specs=(HBM, HBM),
        scratch_shapes=[
            pltpu.VMEM((rows, width), BF16),
            pltpu.VMEM((rank, width), F32),
            pltpu.SemaphoreType.DMA((steps,)),
        ],
        compiler_params=pltpu.CompilerParams(vmem_limit_bytes=8 * MIB),
        name="finish",
    )(merged, left_kept, left_other, inverse, one, two)


def sum_over(value, bits, partner, swap):
    term = value.astype(BF16)
    near = swap(term, bits[0] | partner)
    if len(bits) == 1:
        return term.astype(F32) + near.astype(F32)
    across = swap(term, bits[0] ^ bits[1] ^ partner)
    far = swap(term, bits[1])
    return (term.astype(F32) + near.astype(F32)) + (far.astype(F32) + across.astype(F32))


def per_device(gradient_part, carried_error, query_basis):
    width = gradient_part.shape[3]
    rows = gradient_part.shape[1] * gradient_part.shape[2]
    rank = query_basis.shape[1]
    heads, replicas = lax.axis_size("head"), lax.axis_size("dp")

    def swap(x, bits):
        return lax.ppermute(x, ("head", "dp"), [(i, i ^ bits) for i in range(heads * replicas)])

    gradient, error, left, sent, early = project_sent(
        gradient_part.reshape(rows, width), carried_error.reshape(rows, width), query_basis.T
    )
    mine = project_kept(gradient, error, left, early)
    partner = replicas
    value = mine + swap(sent, partner)
    merged, rounded_kept, rounded_sent = merge(gradient, error)
    rounded_partner = swap(rounded_sent, partner)
    groups = chip_bits(heads, replicas)
    for bits in groups:
        value = sum_over(value, bits, partner, swap)
    terms = factor(rounded_kept, rounded_partner, value, rank)
    for bits in groups:
        for place, bit in enumerate(bits):
            if bit < replicas:
                terms = terms + swap(terms, bit | (0 if place else partner))
    other = swap(value, partner)
    partner_terms = swap(terms, partner)
    run = rows // (2 * FOLD)
    left_kept, gram = prepare([value], (), run, rank, replicas)
    left_other, inverse = prepare([other], (gram,), run, rank, replicas)
    new_error, compressed = finish(merged, left_kept, left_other, inverse, terms, partner_terms)
    return new_error.reshape(gradient_part.shape), compressed.T


def solution(mesh):
    in_specs = (P("dp", None, None, "head"), P("dp", None, None, "head"), P("head", None))
    out_specs = (P("dp", None, None, "head"), P("head", None))

    return jax.shard_map(per_device, mesh=mesh, in_specs=in_specs, out_specs=out_specs, check_vma=False)
```

```python
import functools

import jax
import jax.numpy as jnp
from jax import lax
from jax.experimental import pallas as pl
from jax.experimental.pallas import tpu as pltpu
from jax.sharding import PartitionSpec as P


STREAMS = 1
FOLD = 2
LANES = 128
MIB = 1 << 20
BF16, F32 = jnp.bfloat16, jnp.float32
VMEM = pl.BlockSpec(memory_space=pltpu.VMEM)
HBM = pl.BlockSpec(memory_space=pltpu.HBM)


def split_bf16(x):
    high = x.astype(BF16).astype(F32)
    return high, (x - high).astype(BF16).astype(F32)


def pieces(total, most):
    count = -(-total // most)
    ends = [total * i // count for i in range(count + 1)]
    return [(a * LANES, (b - a) * LANES) for a, b in zip(ends, ends[1:])]


def stream_pieces(run):
    tiles = run // LANES
    ends = [-(-tiles * i // STREAMS) for i in range(STREAMS + 1)]
    return [(a * LANES, (b - a) * LANES) for a, b in zip(ends, ends[1:])]


def chip_bits(heads, replicas):
    bits = [1 << b for b in range((heads * replicas).bit_length() - 1) if 1 << b != replicas]
    return [bits[i : i + 2] for i in range(0, len(bits), 2)]


def kept_half():
    heads, replicas = lax.axis_size("head"), lax.axis_size("dp")
    place = lax.axis_index("head") * replicas + lax.axis_index("dp")
    parity = lax.rem(place // replicas, 2)
    for bits in chip_bits(heads, replicas):
        parity = parity + lax.rem(place // bits[0], 2)
    return lax.rem(parity, 2)


def row_slice(half, fold, run, start, size):
    return pl.ds(pl.multiple_of(half * (FOLD * run) + (fold * run + start), LANES), size)


def product_of(half, fold, start, size, left_ref, g_ref, e_ref):
    run = g_ref.shape[0] // (2 * FOLD)
    rows = left_ref.shape[0] // FOLD
    at = row_slice(half, fold, run, start, size)
    both = jnp.concatenate([g_ref[at, :], e_ref[at, :]], axis=1)
    left = left_ref[fold * rows : (fold + 1) * rows, :]
    product = lax.dot_general(left, both, (((1,), (1,)), ((), ())), preferred_element_type=F32)
    return product[: rows // 2] + product[rows // 2 :]


def early_columns(run):
    return LANES * (run // LANES * 4 // 9)


def project_sent_kernel(rank, g_hbm, e_hbm, q_hbm, g_ref, e_ref, left_ref, *rest):
    sent_ref, early_ref, q_ref, sems, q_sem = rest
    run = g_ref.shape[0] // (2 * FOLD)
    kept = kept_half()
    query_copy = pltpu.make_async_copy(q_hbm, q_ref, q_sem)
    query_copy.start()
    copies = []
    for part, half in enumerate((1 - kept, kept)):
        for fold in range(FOLD):
            at, n = row_slice(half, fold, run, 0, run), len(copies)
            pair = (
                pltpu.make_async_copy(g_hbm.at[at], g_ref.at[at], sems.at[0, n]),
                pltpu.make_async_copy(e_hbm.at[at], e_ref.at[at], sems.at[1, n]),
            )
            for copy in pair:
                copy.start()
            copies.append(pair)
    query_copy.wait()
    high, low = split_bf16(q_ref[...])
    zero = jnp.zeros((rank, LANES), F32)
    for fold in range(FOLD):
        parts = [part if u == fold else zero for part in (high, low) for u in range(FOLD)]
        part = jnp.concatenate(parts, axis=0).astype(BF16)
        rows = part.shape[0]
        left_ref[fold * rows : (fold + 1) * rows, :] = jnp.concatenate([part, part], axis=1)

    def ready(n):
        for copy in copies[n]:
            copy.wait()

    for fold in range(FOLD):
        ready(fold)
        part = product_of(1 - kept, fold, 0, run, left_ref, g_ref, e_ref)
        sent_ref[...] = part if fold == 0 else sent_ref[...] + part
    ready(FOLD)
    early_ref[...] = product_of(kept, 0, 0, early_ref.shape[1], left_ref, g_ref, e_ref)
    for fold in range(1, FOLD):
        ready(FOLD + fold)


def project_sent(gradient, error, query_t):
    rows, width = gradient.shape
    rank = query_t.shape[0]
    run = rows // (2 * FOLD)
    parts = tuple(pltpu.VMEM((FOLD * rank, w), F32) for w in (run, early_columns(run)))
    return pl.pallas_call(
        functools.partial(project_sent_kernel, rank),
        out_shape=(pltpu.VMEM((rows, width), BF16),) * 2 + (pltpu.VMEM((FOLD * 2 * FOLD * rank, 2 * width), BF16),) + parts,
        in_specs=[HBM] * 3,
        out_specs=(VMEM,) * 5,
        scratch_shapes=[
            pltpu.VMEM((rank, width), F32),
            pltpu.SemaphoreType.DMA((2, 2 * FOLD)),
            pltpu.SemaphoreType.DMA,
        ],
        compiler_params=pltpu.CompilerParams(vmem_limit_bytes=4 * MIB),
        name="project_sent",
    )(*(pltpu.with_memory_space_constraint(x, pltpu.HBM) for x in (gradient, error, query_t)))


def project_kept_kernel(g_ref, e_ref, left_ref, early_ref, out_ref):
    kept = kept_half()
    early, run = early_ref.shape[1], out_ref.shape[1]
    out_ref[:, :early] = early_ref[...]
    out_ref[:, early:] = product_of(kept, 0, early, run - early, left_ref, g_ref, e_ref)
    for fold in range(1, FOLD):
        out_ref[...] += product_of(kept, fold, 0, run, left_ref, g_ref, e_ref)


def project_kept(gradient, error, left, early):
    return pl.pallas_call(
        project_kept_kernel,
        out_shape=pltpu.VMEM((early.shape[0], gradient.shape[0] // (2 * FOLD)), F32),
        in_specs=[VMEM] * 4,
        out_specs=VMEM,
        compiler_params=pltpu.CompilerParams(vmem_limit_bytes=4 * MIB),
        name="project_kept",
    )(gradient, error, left, early)


def merge_kernel(g_ref, e_ref, out_ref, kept_ref, sent_ref):
    rows = kept_ref.shape[0]
    kept = kept_half()
    for rounded_ref, half in ((kept_ref, kept), (sent_ref, 1 - kept)):

        def step(i, _):
            to = pl.ds(pl.multiple_of(i * LANES, LANES), LANES)
            at = pl.ds(pl.multiple_of(half * rows + i * LANES, LANES), LANES)
            total = g_ref[at, :].astype(F32) + e_ref[at, :].astype(F32)
            out_ref[at, :] = total
            rounded_ref[to, :] = total.astype(BF16)
            return 0

        lax.fori_loop(0, rows // LANES, step, 0, unroll=2)


def merge(gradient, error):
    rows, width = gradient.shape
    return pl.pallas_call(
        merge_kernel,
        out_shape=(pltpu.VMEM((rows, width), F32),) + (pltpu.VMEM((rows // 2, width), BF16),) * 2,
        in_specs=[VMEM] * 2,
        out_specs=(VMEM,) * 3,
        compiler_params=pltpu.CompilerParams(vmem_limit_bytes=4 * MIB),
        name="merge",
    )(gradient, error)


def by_core(own, partner):
    odd = lax.rem(lax.axis_index("head"), 2) == 1
    return jnp.where(odd, partner, own), jnp.where(odd, own, partner)


def factor_kernel(rank, own_ref, partner_ref, stream_ref, out_ref):
    run = own_ref.shape[0] // FOLD
    sums = [jnp.zeros((2 * FOLD * rank, 2 * LANES), F32) for _ in range(FOLD)]
    for start, size in pieces(run // LANES, 7):
        left = jnp.concatenate(split_bf16(stream_ref[:, start : start + size]), axis=0).astype(BF16)
        for fold in range(FOLD):
            at = pl.ds(fold * run + start, size)
            both = jnp.concatenate([own_ref[at, :], partner_ref[at, :]], axis=1)
            sums[fold] += jnp.dot(left, both, preferred_element_type=F32)
    total = jnp.zeros((rank, 2 * LANES), F32)
    for fold in range(FOLD):
        whole = sums[fold][: FOLD * rank] + sums[fold][FOLD * rank :]
        total += whole[fold * rank : (fold + 1) * rank]
    out_ref[...] = jnp.concatenate(by_core(total[:, :LANES], total[:, LANES:]), axis=0)


def factor(own, partner, stream, rank):
    return pl.pallas_call(
        functools.partial(factor_kernel, rank),
        out_shape=pltpu.VMEM((2 * rank, own.shape[1]), F32),
        in_specs=[VMEM] * 3,
        out_specs=VMEM,
        compiler_params=pltpu.CompilerParams(vmem_limit_bytes=4 * MIB),
        name="factor",
    )(own, partner, stream)


def solve(rank, replicas, gram, out_ref):
    lower, reciprocal = {}, {}
    for j in range(rank):
        for i in range(j, rank):
            value = gram(i, j)
            for k in range(j):
                value = value - lower[i, k] * lower[j, k]
            if i == j:
                reciprocal[j] = 1.0 / jnp.sqrt(value)
            else:
                lower[i, j] = value * reciprocal[j]
    inverse = {}
    for j in range(rank):
        inverse[j, j] = reciprocal[j]
        for i in range(j + 1, rank):
            value = lower[i, j] * inverse[j, j]
            for k in range(j + 1, i):
                value = value + lower[i, k] * inverse[k, j]
            inverse[i, j] = -value * reciprocal[i]
    zero = jnp.zeros((1, LANES), F32)
    for k in range(rank):
        for j in range(rank):
            column = inverse[j, k] * (1.0 / replicas) if j >= k else zero
            row = inverse[k, j] if k >= j else zero
            out_ref[8 * k + j : 8 * k + j + 1, :] = column
            out_ref[8 * (rank + k) + j : 8 * (rank + k) + j + 1, :] = row


def prepare_kernel(rank, replicas, other, *rest):
    streams, so_far, (left_ref, out_ref) = rest[:STREAMS], rest[STREAMS:-2], rest[-2:]
    rows = FOLD * rank
    run = left_ref.shape[0]
    grams = [jnp.zeros((rows, LANES), F32) for _ in range(rank)]
    for s, (base, width) in enumerate(stream_pieces(run)):
        for start, size in pieces(width // LANES, 7):
            part = streams[s][:, start : start + size]
            high, low = split_bf16(part)
            left = jnp.concatenate([high, low, high, jnp.zeros_like(part)], axis=0)
            left_ref[base + start : base + start + size, :] = left.T.astype(BF16)
            for d in range(rank):
                product = part * (part if d == 0 else pltpu.roll(part, d, 0))
                for c in range(0, size, LANES):
                    grams[d] += product[:, c : c + LANES]
    sums = []
    for d in range(rank):
        value = jnp.broadcast_to(jnp.sum(grams[d], axis=1, keepdims=True), (rows, LANES))
        sums.append(value + so_far[0][d * rows : (d + 1) * rows, :] if so_far else value)
    if not other:
        for d in range(rank):
            out_ref[d * rows : (d + 1) * rows, :] = sums[d]
        return

    def gram(i, j):
        return sum(sums[i - j][fold * rank + i : fold * rank + i + 1] for fold in range(FOLD))

    solve(rank, replicas, gram, out_ref)


def prepare(streams, so_far, run, rank, replicas):
    other = len(so_far) > 0
    out_rows = 16 * rank if other else rank * FOLD * rank
    return pl.pallas_call(
        functools.partial(prepare_kernel, rank, replicas, other),
        out_shape=(pltpu.VMEM((run, 4 * FOLD * rank), BF16), pltpu.VMEM((out_rows, LANES), F32)),
        in_specs=[VMEM] * (STREAMS + len(so_far)),
        out_specs=(VMEM,) * 2,
        compiler_params=pltpu.CompilerParams(vmem_limit_bytes=8 * MIB),
        name="prepare_other" if other else "prepare_kept",
    )(*streams, *so_far)


def finish_kernel(rank, merged_ref, kept_ref, other_ref, inverse_ref, own_ref, same_ref, cross_ref, core_ref, new_hbm, factor_hbm, staged, factor_ref, sems):
    run = kept_ref.shape[0]
    kept = kept_half()
    raw = (own_ref[...] + core_ref[...]) + (same_ref[...] + cross_ref[...])
    raw, _ = by_core(raw[:rank], raw[rank:])
    small = sum(inverse_ref[8 * k : 8 * k + rank, :] * raw[k : k + 1] for k in range(rank))
    factor_ref[...] = small
    copies = [pltpu.make_async_copy(factor_ref, factor_hbm, sems.at[0])]
    copies[0].start()
    weight = sum(inverse_ref[8 * (rank + k) : 8 * (rank + k) + rank, :] * small[k : k + 1] for k in range(rank))
    high, low = split_bf16(weight)
    zero = jnp.zeros((rank, LANES), F32)
    right = []
    for fold in range(FOLD):
        parts = [part if u == fold else zero for part in (high, high, low, zero) for u in range(FOLD)]
        right.append(jnp.concatenate(parts, axis=0).astype(BF16))
    for left_ref, half in ((kept_ref, kept), (other_ref, 1 - kept)):
        for start, size in pieces(run // LANES, 7):
            for fold in range(FOLD):
                at = row_slice(half, fold, run, start, size)
                product = jnp.dot(left_ref[start : start + size, :], right[fold], preferred_element_type=F32)
                staged[at, :] = (merged_ref[at, :] - product).astype(BF16)
                copy = pltpu.make_async_copy(staged.at[at], new_hbm.at[at], sems.at[len(copies)])
                copy.start()
                copies.append(copy)
    for copy in copies:
        copy.wait()


def finish(merged, left_kept, left_other, inverse, own, same, cross, core):
    rows, width = merged.shape
    rank = own.shape[0] // 2
    steps = 1 + 2 * FOLD * len(pieces(left_kept.shape[0] // LANES, 7))
    return pl.pallas_call(
        functools.partial(finish_kernel, rank),
        out_shape=(jax.ShapeDtypeStruct((rows, width), BF16), jax.ShapeDtypeStruct((rank, width), F32)),
        in_specs=[VMEM] * 8,
        out_specs=(HBM, HBM),
        scratch_shapes=[
            pltpu.VMEM((rows, width), BF16),
            pltpu.VMEM((rank, width), F32),
            pltpu.SemaphoreType.DMA((steps,)),
        ],
        compiler_params=pltpu.CompilerParams(vmem_limit_bytes=8 * MIB),
        name="finish",
    )(merged, left_kept, left_other, inverse, own, same, cross, core)


def sum_over(value, bits, partner, swap):
    term = value.astype(BF16)
    near = swap(term, bits[0] | partner)
    if len(bits) == 1:
        return term.astype(F32) + near.astype(F32)
    across = swap(term, bits[0] ^ bits[1] ^ partner)
    far = swap(term, bits[1])
    return (term.astype(F32) + near.astype(F32)) + (far.astype(F32) + across.astype(F32))


def per_device(gradient_part, carried_error, query_basis):
    width = gradient_part.shape[3]
    rows = gradient_part.shape[1] * gradient_part.shape[2]
    rank = query_basis.shape[1]
    heads, replicas = lax.axis_size("head"), lax.axis_size("dp")

    def swap(x, bits):
        return lax.ppermute(x, ("head", "dp"), [(i, i ^ bits) for i in range(heads * replicas)])

    gradient, error, left, sent, early = project_sent(
        gradient_part.reshape(rows, width), carried_error.reshape(rows, width), query_basis.T
    )
    mine = project_kept(gradient, error, left, early)
    partner = replicas
    value = mine + swap(sent.astype(BF16), partner).astype(F32)
    merged, rounded_kept, rounded_sent = merge(gradient, error)
    rounded_partner = swap(rounded_sent, partner)
    groups = chip_bits(heads, replicas)
    for bits in groups:
        value = sum_over(value, bits, partner, swap)
    terms = factor(rounded_kept, rounded_partner, value, rank)
    for bits in groups:
        for place, bit in enumerate(bits):
            if 1 < bit < replicas:
                terms = terms + swap(terms, bit | (0 if place else partner))
    received = []
    for bits in (1, 1 | partner, partner):
        received.append(swap(terms, bits))
    other = swap(value, partner)
    run = rows // (2 * FOLD)
    left_kept, gram = prepare([value], (), run, rank, replicas)
    left_other, inverse = prepare([other], (gram,), run, rank, replicas)
    new_error, compressed = finish(merged, left_kept, left_other, inverse, terms, *received)
    return new_error.reshape(gradient_part.shape), compressed.T


def solution(mesh):
    in_specs = (P("dp", None, None, "head"), P("dp", None, None, "head"), P("head", None))
    out_specs = (P("dp", None, None, "head"), P("head", None))

    return jax.shard_map(per_device, mesh=mesh, in_specs=in_specs, out_specs=out_specs, check_vma=False)
```
